32 devices in a mesh: row: 4 (over y, x), col: 8 (over z, core).
Axes of the slice: x: 2, y: 2, z: 4, core: 2. Of those that a mesh axis runs over, the one named last changes fastest.
Arguments:
- out_grad: bfloat16 [4096, 512], P('col', 'row'), may hold values from -6 to 6
- node_in: bfloat16 [4096, 512], P(('row', 'col')), may hold values from -0.09375 to 0.09375
- weights: bfloat16 [3, 512, 512], replicated, may hold values from -0.25 to 0.25
- tile_vals: bfloat16 [3, 8, 4, 32, 128, 128], P(None, 'col', 'row'), may hold values from -0.15625 to 0.15625
- tile_rows: int32 [3, 8, 4, 32], P(None, 'col', 'row'), may hold values from 0 to 3
- tile_cols: int32 [3, 8, 4, 32], P(None, 'col', 'row'), may hold values from 0 to 7
- tile_count: int32 [3, 8, 4], P(None, 'col', 'row'), may hold values from 1 to 32, as said below
Outputs:
- d_nodes: bfloat16 [4096, 512], P(('row', 'col'))
- d_weights: float32 [3, 512, 512], replicated
The draws below stay inside these ranges and needn't reach their ends.
Inputs may be any that keep to these rules, and one draw needn't show every extreme that they name: Only the first tile_count slots of a block's list hold tiles; later slots are ignored. In every relation some block uses all 32 slots. `tile_rows`: coordinates may repeat within a block's list; such tiles add.
All inputs are finite; a program needn't handle non-finite values.
Results may differ from the reference program's by a relative error of at most 0.005.
Values may be sent and summed in bfloat16 or wider, within the bound.
A program may use at most 256 MiB of HBM per device.

```python
import jax
import jax.numpy as jnp
from jax import lax

D = 512
R = 3
TILE = 128
N_DEV = 128
CAP = 32
ROW_GROUPS = 4
COL_GROUPS = 8
NODES = 4096
TR = 4
TC = 8


def draw_tile_count(key, part):
    grid_shape = (R, COL_GROUPS, ROW_GROUPS)
    levels = jax.random.randint(jax.random.fold_in(key, 11), grid_shape, 1, 9)
    counts = jnp.maximum(1, CAP * levels * levels // 64)
    full_device = jax.random.randint(jax.random.fold_in(key, 12), (R,), 0, COL_GROUPS * ROW_GROUPS)
    flat_counts = counts.reshape(R, COL_GROUPS * ROW_GROUPS)
    chosen = jnp.arange(COL_GROUPS * ROW_GROUPS)[None, :] == full_device[:, None]
    flat_counts = jnp.where(chosen, CAP, flat_counts)
    return flat_counts.reshape(grid_shape).astype(jnp.int32)


def touch_ends(array, own_key, least, largest):
    extent = array.shape
    place = [jax.random.randint(jax.random.fold_in(own_key, axis), (), 0, extent[axis]) for axis in range(len(extent))]
    array = array.at[tuple(place)].set(least)
    longest = extent.index(max(extent))
    place[longest] = (place[longest] + 1) % extent[longest]
    return array.at[tuple(place)].set(largest)


def shard_levels(rng, shape, cuts, low, largest):
    def one(position, blocks):
        draws = jax.random.uniform(jax.random.fold_in(jax.random.fold_in(rng, 6), position), (blocks,), jnp.float32, low / len(cuts), largest / len(cuts))
        return jnp.repeat(jnp.exp(draws), shape[position] // blocks).reshape((-1,) + (1,) * (len(shape) - position - 1))

    loudness = one(*cuts[0])
    for cut in cuts[1:]:
        loudness = loudness * one(*cut)
    return loudness


def bell_draw(stream_key, dims, spread, most, split=(), held_as=jnp.bfloat16):
    drawn = spread * jax.random.normal(stream_key, dims, jnp.float32)
    if split:
        drawn = drawn * shard_levels(stream_key, dims, split, -0.22, 0.18)
    return jnp.clip(drawn, -most, most).astype(held_as)


def setup_inputs(seed: int = 0) -> dict:
    streams_of = jax.random.split(jax.random.key(seed), 8)
    out_grad = bell_draw(streams_of[0], (NODES, D), 1.0, 6.0, ((0, 8), (1, 4)))
    node_in = bell_draw(streams_of[1], (NODES, D), NODES ** -0.5, 0.09375, ((0, 32),))
    weights = bell_draw(streams_of[2], (R, D, D), D ** -0.5, 0.25)
    tile_vals = bell_draw(streams_of[3], (R, COL_GROUPS, ROW_GROUPS, CAP, TILE, TILE), (CAP * COL_GROUPS * 2 * TILE // (5 * TC)) ** -0.5, 0.15625, ((1, 8), (2, 4)))
    tile_rows = touch_ends(jax.random.randint(streams_of[4], (R, COL_GROUPS, ROW_GROUPS, CAP), 0, TR), jax.random.fold_in(streams_of[4], 1), 0, TR - 1).astype(jnp.int32)
    tile_cols = touch_ends(jax.random.randint(streams_of[5], (R, COL_GROUPS, ROW_GROUPS, CAP), 0, TC), jax.random.fold_in(streams_of[5], 1), 0, TC - 1).astype(jnp.int32)
    tile_count = draw_tile_count(jax.random.fold_in(streams_of[7], 71), 0)
    return {"out_grad": out_grad, "node_in": node_in, "weights": weights, "tile_vals": tile_vals, "tile_rows": tile_rows, "tile_cols": tile_cols, "tile_count": tile_count}


def block_products(operand, tile_block, row_ids, col_ids, count_now, block_index):
    group_col = block_index // ROW_GROUPS
    group_row = block_index % ROW_GROUPS
    lanes = jnp.arange(TILE, dtype=jnp.int32)
    source_ids = (group_col * (N_DEV * ROW_GROUPS) + row_ids[:, None] * TILE + lanes[None, :]).astype(jnp.int32)
    sources = jnp.take(operand, source_ids.reshape(-1), axis=0).reshape(CAP, TILE, 2 * D)
    live = (jnp.arange(CAP, dtype=jnp.int32) < count_now).astype(jnp.float32)
    products = jnp.einsum("skt,skd->std", tile_block.astype(jnp.float32), sources.astype(jnp.float32), precision=lax.Precision.HIGHEST)
    products = products * live[:, None, None]
    target_ids = (group_row * (N_DEV * COL_GROUPS) + col_ids[:, None] * TILE + lanes[None, :]).astype(jnp.int32)
    return target_ids.reshape(-1), products.reshape(CAP * TILE, 2 * D)


def reference(out_grad, node_in, weights, tile_vals, tile_rows, tile_cols, tile_count):
    blocks = COL_GROUPS * ROW_GROUPS
    block_ids = jnp.arange(blocks, dtype=jnp.int32)
    mixed_total = jnp.zeros((NODES, D), jnp.float32)
    weight_grads = []
    inputs_wide = node_in.astype(jnp.float32)
    for relation in range(R):
        premixed = jnp.dot(out_grad, weights[relation].T, preferred_element_type=jnp.float32).astype(jnp.bfloat16)
        operand = jnp.concatenate([out_grad, premixed], axis=1)

        def block_step(summed, inputs):
            target_ids, products = block_products(operand, inputs[0], inputs[1], inputs[2], inputs[3], inputs[4])
            return summed.at[target_ids].add(products), None

        scanned = (tile_vals[relation].reshape(blocks, CAP, TILE, TILE), tile_rows[relation].reshape(blocks, CAP), tile_cols[relation].reshape(blocks, CAP), tile_count[relation].reshape(blocks), block_ids)
        start_sums = jnp.zeros((NODES, 2 * D), jnp.float32)
        summed, ignored = lax.scan(block_step, start_sums, scanned)
        weight_grads.append(jnp.dot(inputs_wide.T, summed[:, :D], precision=lax.Precision.HIGHEST))
        mixed_total = mixed_total + summed[:, D:]
    return mixed_total.astype(jnp.bfloat16), jnp.stack(weight_grads)
```

```python
import functools

import jax
import jax.numpy as jnp
from jax import lax
from jax.experimental import pallas as pl
from jax.experimental.pallas import tpu as pltpu
from jax.sharding import PartitionSpec as P

MESH = pl.DeviceIdType.MESH
F32 = jnp.float32
BF16 = jnp.bfloat16
I32 = jnp.int32
HALVES = 2
scope = jax.named_scope


def reduce_order(chunks):
    link, hop = 1.4, 3.3
    events = []
    for k in range(chunks):
        t = link * k
        for stage, at in ((2, t), (3, t + hop), (4, t + 2 * hop), (5, t + 3 * hop)):
            events.append((at, stage, k))
    return [(stage, k) for _, stage, k in sorted(events)]


def main_kernel(
    nr, nc, relations, tile_cols_n,
    rows_hbm, cols_hbm, count_hbm, vals_hbm, grad_hbm, nodes_hbm, w_hbm,
    dn_ref, ag_ref,
    rows_v, cols_v, count_v, table_v, table_s, vals, chain, gslot, g, w, a, xall, pt,
    nsend, nrecv, ndst, nfin, pbuf, crecv, precv, zbuf, zrecv,
    small_sem, val_sem, load_sem, gs, gr, xs, xr, fs, fr, ns, nrs, nzs, nzr, nfs, nfr,
    cs, cr, ps, pr, zs, zr, azs, azr, aps, apr, acs, acr,
):
    nz = nc // 2
    cap, tile = vals.shape[1], vals.shape[2]
    tn, width = gslot.shape[1], gslot.shape[2]
    nd = nodes_hbm.shape[0]
    f = w_hbm.shape[1]
    tile_rows_n = tn // tile
    half = f // HALVES
    plane_rows = pbuf.shape[3]
    piece = zbuf.shape[2]
    lanes_f = f // tile
    chunks = relations * HALVES
    me_r = lax.axis_index("row")
    me_c = lax.axis_index("col")
    z = me_c // 2
    core = me_c % 2
    sibling = {"col": z * 2 + 1 - core}
    lead = core == 1
    other = core == 0

    def row_peer(d):
        return {"row": lax.rem(me_r + d, nr)}

    def z_peer(d):
        return {"col": lax.rem(z + d, nz) * 2 + core}

    def remote(src, dst, send, recv, dev):
        return pltpu.make_async_remote_copy(
            src_ref=src, dst_ref=dst, send_sem=send, recv_sem=recv, device_id=dev, device_id_type=MESH
        )

    def x_slot(k):
        return xall.at[pl.ds(pl.multiple_of(k * nd, nd), nd), :]

    with scope("entry"):
        barrier = pltpu.get_barrier_semaphore()
        for d in range(1, nr):
            pl.semaphore_signal(barrier, inc=1, device_id=row_peer(d), device_id_type=MESH)
        for d in range(1, nz):
            pl.semaphore_signal(barrier, inc=1, device_id=z_peer(d), device_id_type=MESH)
        pl.semaphore_signal(barrier, inc=1, device_id=sibling, device_id_type=MESH)

        small = [
            pltpu.make_async_copy(rows_hbm, rows_v, small_sem.at[0]),
            pltpu.make_async_copy(cols_hbm, cols_v, small_sem.at[1]),
            pltpu.make_async_copy(count_hbm, count_v, small_sem.at[2]),
        ]
        load_g = pltpu.make_async_copy(grad_hbm, gslot.at[me_r], load_sem.at[0])
        load_x = pltpu.make_async_copy(nodes_hbm, x_slot(me_c), load_sem.at[1])
        load_w = pltpu.make_async_copy(w_hbm, w, load_sem.at[2])
        load_vals = [pltpu.make_async_copy(vals_hbm.at[r], vals.at[r], val_sem.at[r]) for r in range(relations)]
        load_g.start()
        load_x.start()
        for c in small:
            c.start()
        for c in load_vals:
            c.start()
        load_w.start()

    with scope("tables"):
        for c in small:
            c.wait()
        spread = table_v.shape[1]
        slot_lane = lax.broadcasted_iota(I32, (1, cap), 1)
        slot_row = lax.broadcasted_iota(I32, (cap, cap), 0)
        slot_col = lax.broadcasted_iota(I32, (cap, cap), 1)
        place_row = lax.broadcasted_iota(I32, (cap, spread), 0)
        place_col = lax.broadcasted_iota(I32, (cap, spread), 1)
        for r in range(relations):
            key = rows_v[r, 0] * tile_cols_n + cols_v[r, 0]
            key = jnp.where(slot_lane < count_v[0:1, r : r + 1], key, -1)
            down = jnp.max(jnp.where(slot_row == slot_col, jnp.broadcast_to(key, (cap, cap)), -1), axis=1, keepdims=True)
            same = (down == key) & (slot_row < slot_col)
            before = jnp.max(jnp.where(same, slot_row + 1, 0), axis=0, keepdims=True)
            last = jnp.max(jnp.where(down == place_col, place_row + 1, 0), axis=0, keepdims=True)
            table_v[r : r + 1, 0:cap] = before
            table_v[relations + r : relations + r + 1, :] = last
        load_table = pltpu.make_async_copy(table_v, table_s, small_sem.at[3])
        load_table.start()

    with scope("barrier"):
        pl.semaphore_wait(barrier, nr - 1 + nz - 1 + 1)
        load_g.wait()
    with scope("sends"):
        mine = gslot.at[me_r]
        g_copies = [remote(mine, mine, gs.at[d - 1], gr.at[d - 1], row_peer(d)) for d in range(1, nr)]
        for c in g_copies:
            c.start()
        load_x.wait()
        own_x = x_slot(me_c)
        x_copies = [remote(own_x, own_x, xs.at[d - 1], xr.at[d - 1], z_peer(d)) for d in range(1, nz)]
        for c in x_copies:
            c.start()
        f_copies = [remote(own_x, own_x, fs.at[0], fr.at[0], sibling)]
        f_copies[0].start()

    with scope("chain"):
        load_table.wait()
        for c in load_vals:
            c.wait()
        for r in range(relations):
            chain[r, 0] = jnp.zeros((tile, tile), F32)

        def link(s, carry):
            for r in range(relations):
                chain[r, s + 1] = chain[r, table_s[r, s]] + vals[r, s].astype(F32)
            return carry

        lax.fori_loop(0, cap, link, 0)

    with scope("place"):

        def place(i, carry):
            def one(j, inner):
                for r in range(relations):
                    rows = pl.ds(pl.multiple_of(r * tn + i * tile, tile), tile)
                    cols = pl.ds(pl.multiple_of(j * tile, tile), tile)
                    a[rows, cols] = chain[r, table_s[relations + r, i * tile_cols_n + j]].astype(BF16)
                return inner

            return lax.fori_loop(0, tile_cols_n, one, carry)

        lax.fori_loop(0, tile_rows_n, place, 0)

    def forward(d):
        x_copies[d - 1].wait_recv()
        slot = x_slot(lax.rem(z + nz - d, nz) * 2 + core)
        c = remote(slot, slot, fs.at[d], fr.at[d], sibling)
        c.start()
        f_copies.append(c)

    def y_block(d):
        both = pl.ds(pl.multiple_of(lax.rem(z + nz - d, nz) * 2 * nd, 2 * nd), 2 * nd)
        for r in range(relations):
            part = jnp.dot(a[r * tn : (r + 1) * tn, both], xall[both, :], preferred_element_type=F32)
            for i in range(tile_rows_n):
                for j in range(lanes_f):
                    b = part[i * tile : (i + 1) * tile, j * tile : (j + 1) * tile]
                    at = i * lanes_f + j
                    if d > 0:
                        b = b + chain[r, at]
                    if d < nz - 1:
                        chain[r, at] = b
                    else:
                        pt[j * tile : (j + 1) * tile, r * tn + i * tile : r * tn + (i + 1) * tile] = b.astype(BF16).T

    with scope("y0"):
        f_copies[0].wait_recv()
        y_block(0)
    with scope("fwd1"):
        if nz > 1:
            forward(1)
    with scope("waitg"):
        load_w.wait()
        for c in g_copies:
            c.wait_recv()
    with scope("premix"):
        for k in range(nr):
            g[:, k * width : (k + 1) * width] = gslot[k]
        for r in range(relations):
            pt[:, r * tn : (r + 1) * tn] = lax.dot_general(
                w[r], g[...], (((1,), (1,)), ((), ())), preferred_element_type=F32
            ).astype(BF16)
    with scope("fwd2"):
        if nz > 2:
            forward(2)

    def mix(k, carry):
        cols = pl.ds(pl.multiple_of(k * 2 * nd, 2 * nd), 2 * nd)
        both = jnp.dot(pt[...], a[:, cols], preferred_element_type=F32)
        nsend[k, 0] = both[:, :nd].astype(BF16)
        nsend[k, 1] = both[:, nd:].astype(BF16)
        return carry

    with scope("mix"):
        lax.fori_loop(0, nz, mix, 0)

        @pl.when(lead)
        def _():
            remote(nsend, nrecv, ns.at[0], nrs.at[0], sibling).start()

    with scope("fwd3"):
        for d in range(3, nz):
            forward(d)

    for d in range(1, nz):
        with scope(f"y{d}"):
            f_copies[d].wait_recv()
            y_block(d)

    def n_core():
        return remote(nsend, nrecv, ns.at[0], nrs.at[0], sibling)

    def own_dn():
        return remote(nfin, dn_ref, nfs.at[0], nfr.at[0], sibling)

    def dn_copies():
        return [
            remote(nsend.at[lax.rem(z + d, nz)], ndst.at[d - 1], nzs.at[d - 1], nzr.at[d - 1], z_peer(d))
            for d in range(1, nz)
        ]

    def c_copy(k):
        r, h = k // HALVES, k % HALVES
        return remote(pbuf.at[r, h], crecv.at[r, h], cs.at[k], cr.at[k], sibling)

    def p_copies(k):
        r, h = k // HALVES, k % HALVES
        return [
            remote(
                pbuf.at[r, h, lax.rem(me_r + d, nr)], precv.at[k, d - 1],
                ps.at[k, d - 1], pr.at[k, d - 1], row_peer(d),
            )
            for d in range(1, nr)
        ]

    def z_copies(k):
        return [
            remote(
                zbuf.at[k, lax.rem(z + d, nz)], zrecv.at[k, d - 1],
                zs.at[k, d - 1], zr.at[k, d - 1], z_peer(d),
            )
            for d in range(1, nz)
        ]

    def za_copies(k):
        part = ag_ref.at[k // HALVES, k % HALVES, me_r, z]
        return [remote(part, part, azs.at[k, d - 1], azr.at[k, d - 1], z_peer(d)) for d in range(1, nz)]

    def pa_copies(k):
        part = ag_ref.at[k // HALVES, k % HALVES, me_r]
        return [remote(part, part, aps.at[k, d - 1], apr.at[k, d - 1], row_peer(d)) for d in range(1, nr)]

    def ca_copy(k, d):
        part = ag_ref.at[k // HALVES, k % HALVES, lax.rem(me_r + nr - d, nr)]
        return remote(part, part, acs.at[k, d], acr.at[k, d], sibling)

    def begin(copies):
        for c in copies:
            c.start()

    def arrived(copies):
        for c in copies:
            c.wait_recv()

    def left(copies):
        for c in copies:
            c.wait_send()

    def held_rows(r, h, q):
        first = h * half + q * plane_rows
        block, off = first // tile, first % tile
        assert off + plane_rows <= tile
        return jnp.concatenate(
            [chain[r, block * lanes_f + j, off : off + plane_rows, :] for j in range(lanes_f)], axis=1
        )

    def terms(k):
        r, h = k // HALVES, k % HALVES
        v = jnp.dot(pt[h * half : (h + 1) * half, r * tn : (r + 1) * tn], g[...], preferred_element_type=F32)
        for i in range(half // tile):
            for j in range(lanes_f):
                at = (h * (half // tile) + i) * lanes_f + j
                chain[r, at] = v[i * tile : (i + 1) * tile, j * tile : (j + 1) * tile]

        @pl.when(other)
        def _():
            for q in range(nr):
                pbuf[r, h, q] = held_rows(r, h, q).astype(BF16)
            c_copy(k).start()

    def plane_scatter(k):
        r, h = k // HALVES, k % HALVES
        c_copy(k).wait_recv()
        for q in range(nr):
            pbuf[r, h, q] = (held_rows(r, h, q) + crecv[r, h, q].astype(F32)).astype(BF16)
        begin(p_copies(k))

    def z_scatter(k):
        r, h = k // HALVES, k % HALVES
        arrived(p_copies(k))
        for q in range(nz):
            rows = slice(q * piece, (q + 1) * piece)
            part = pbuf[r, h, me_r, rows, :].astype(F32)
            for d in range(1, nr):
                part = part + precv[k, d - 1, rows, :].astype(F32)
            zbuf[k, q] = part.astype(BF16)
        begin(z_copies(k))

    def z_gather(k):
        arrived(z_copies(k))
        final = zbuf[k, z].astype(F32)
        for d in range(1, nz):
            final = final + zrecv[k, d - 1].astype(F32)
        ag_ref[k // HALVES, k % HALVES, me_r, z] = final.astype(BF16)
        begin(za_copies(k))

    def plane_gather(k):
        arrived(za_copies(k))
        begin(pa_copies(k))
        ca_copy(k, 0).start()

    def core_gather(k):
        copies = pa_copies(k)
        for d in range(1, nr):
            copies[d - 1].wait_recv()
            ca_copy(k, d).start()

    behind = 3
    for k in range(chunks):
        with scope(f"terms{k}"):
            terms(k)
        if k >= behind:
            with scope(f"s1_{k - behind}"):

                @pl.when(lead)
                def _():
                    plane_scatter(k - behind)

    @pl.when(lead)
    def _():
        for k in range(max(chunks - behind, 0), chunks):
            with scope(f"s1_{k}"):
                plane_scatter(k)
        stages = {2: z_scatter, 3: z_gather, 4: plane_gather, 5: core_gather}
        for stage, k in reduce_order(chunks):
            with scope(f"s{stage}_{k}"):
                stages[stage](k)
        with scope("end"):
            own_dn().wait_recv()
            n_core().wait_send()
            for k in range(chunks):
                left(p_copies(k) + z_copies(k) + za_copies(k) + pa_copies(k))
                left([ca_copy(k, d) for d in range(nr)])

    @pl.when(other)
    def _():
        with scope("dn_wait"):
            n_core().wait_recv()

        def combine(d, carry):
            k = lax.rem(z + d, nz)
            nsend[k] = (nsend[k].astype(F32) + nrecv[k].astype(F32)).astype(BF16)
            return carry

        with scope("dn_comb"):
            lax.fori_loop(1, nz, combine, 0)
            begin(dn_copies())
        with scope("dn_recv"):
            arrived(dn_copies())
        with scope("dn_fin"):
            for part in range(2):
                own = nsend[z, part].astype(F32) + nrecv[z, part].astype(F32)
                for d in range(1, nz):
                    own = own + ndst[d - 1, part].astype(F32)
                done = own.T.astype(BF16)
                if part == 0:
                    dn_ref[...] = done
                else:
                    nfin[...] = done
            own_dn().start()
        with scope("oend"):
            for k in range(chunks):
                arrived([ca_copy(k, d) for d in range(nr)])
            left([c_copy(k) for k in range(chunks)])
            left(dn_copies())
            own_dn().wait_send()

    left(g_copies + x_copies + f_copies)


def widen_kernel(dn_ref, dw_ref, dn_out, dw_out, wide, out_sem):
    parts, rows = wide.shape[0], wide.shape[1]
    stores = [
        pltpu.make_async_copy(wide.at[k], dw_out.at[k * rows : (k + 1) * rows, :], out_sem.at[k])
        for k in range(parts)
    ]
    stores.append(pltpu.make_async_copy(dn_ref, dn_out, out_sem.at[parts]))
    stores[parts].start()
    for k in range(parts):
        wide[k] = dw_ref[k * rows : (k + 1) * rows, :].astype(F32)
        stores[k].start()
    for c in stores:
        c.wait()


def widen(d_nodes, gathered):
    total, f = gathered.shape
    parts = 6 if total % 96 == 0 else 1
    rows = total // parts
    hbm = pl.BlockSpec(memory_space=pltpu.HBM)
    vmem = pl.BlockSpec(memory_space=pltpu.VMEM)
    return pl.pallas_call(
        widen_kernel,
        in_specs=[vmem, vmem],
        out_specs=(hbm, hbm),
        out_shape=(
            jax.ShapeDtypeStruct(d_nodes.shape, BF16),
            jax.ShapeDtypeStruct(gathered.shape, F32),
        ),
        scratch_shapes=[
            pltpu.VMEM((parts, rows, f), F32),
            pltpu.SemaphoreType.DMA((parts + 1,)),
        ],
    )(
        pltpu.with_memory_space_constraint(d_nodes, pltpu.VMEM),
        pltpu.with_memory_space_constraint(gathered, pltpu.VMEM),
    )


def body(nr, nc, out_grad, node_in, weights, tile_vals, tile_rows, tile_cols, tile_count):
    relations, f = weights.shape[0], weights.shape[1]
    cap, tile = tile_vals.shape[3], tile_vals.shape[4]
    tn, width = out_grad.shape
    nd = node_in.shape[0]
    sn = nd * nc
    nz = nc // 2
    half = f // HALVES
    plane_rows = half // nr
    piece = plane_rows // nz
    chunks = relations * HALVES
    places = (tn // tile) * (sn // tile)
    spread = -(-max(places, cap) // 128) * 128
    blocks = max(cap + 1, (tn // tile) * (f // tile), (f // tile) ** 2)
    dma = lambda *n: pltpu.SemaphoreType.DMA(n)
    hbm = pl.BlockSpec(memory_space=pltpu.HBM)
    vmem = pl.BlockSpec(memory_space=pltpu.VMEM)
    d_nodes, gathered = pl.pallas_call(
        functools.partial(main_kernel, nr, nc, relations, sn // tile),
        out_shape=(
            pltpu.VMEM((nd, f), BF16),
            pltpu.VMEM((relations, HALVES, nr, nz, piece, f), BF16),
        ),
        in_specs=[hbm] * 7,
        out_specs=(vmem, vmem),
        scratch_shapes=[
            pltpu.VMEM(tile_rows.shape, I32),
            pltpu.VMEM(tile_cols.shape, I32),
            pltpu.VMEM((1, relations), I32),
            pltpu.VMEM((-(-2 * relations // 8) * 8, spread), I32),
            pltpu.SMEM((-(-2 * relations // 8) * 8, spread), I32),
            pltpu.VMEM((relations, cap, tile, tile), BF16),
            pltpu.VMEM((relations, blocks, tile, tile), F32),
            pltpu.VMEM((nr, tn, width), BF16),
            pltpu.VMEM((tn, f), BF16),
            pltpu.VMEM(weights.shape, BF16),
            pltpu.VMEM((relations * tn, sn), BF16),
            pltpu.VMEM((sn, f), BF16),
            pltpu.VMEM((f, relations * tn), BF16),
            pltpu.VMEM((nz, 2, f, nd), BF16),
            pltpu.VMEM((nz, 2, f, nd), BF16),
            pltpu.VMEM((nz - 1, 2, f, nd), BF16),
            pltpu.VMEM((nd, f), BF16),
            pltpu.VMEM((relations, HALVES, nr, plane_rows, f), BF16),
            pltpu.VMEM((relations, HALVES, nr, plane_rows, f), BF16),
            pltpu.VMEM((chunks, nr - 1, plane_rows, f), BF16),
            pltpu.VMEM((chunks, nz, piece, f), BF16),
            pltpu.VMEM((chunks, nz - 1, piece, f), BF16),
            dma(4), dma(relations), dma(3),
            dma(nr - 1), dma(nr - 1),
            dma(nz - 1), dma(nz - 1),
            dma(nz), dma(nz),
            dma(1), dma(1),
            dma(nz - 1), dma(nz - 1),
            dma(1), dma(1),
            dma(chunks), dma(chunks),
            dma(chunks, nr - 1), dma(chunks, nr - 1),
            dma(chunks, nz - 1), dma(chunks, nz - 1),
            dma(chunks, nz - 1), dma(chunks, nz - 1),
            dma(chunks, nr - 1), dma(chunks, nr - 1),
            dma(chunks, nr), dma(chunks, nr),
        ],
        compiler_params=pltpu.CompilerParams(
            collective_id=0, has_side_effects=True, vmem_limit_bytes=63000 * 1024
        ),
    )(
        tile_rows,
        tile_cols,
        tile_count.reshape(1, relations),
        tile_vals.reshape(relations, cap, tile, tile),
        out_grad,
        node_in,
        weights,
    )
    d_nodes, d_weights = widen(d_nodes, gathered.reshape(relations * f, f))
    return d_nodes, d_weights.reshape(relations, f, f)


def solution(mesh):
    return jax.shard_map(
        functools.partial(body, mesh.shape["row"], mesh.shape["col"]),
        mesh=mesh,
        in_specs=(
            P("col", "row"),
            P(("row", "col"), None),
            P(),
            P(None, "col", "row", None, None, None),
            P(None, "col", "row", None),
            P(None, "col", "row", None),
            P(None, "col", "row"),
        ),
        out_specs=(P(("row", "col"), None), P()),
        check_vma=False,
    )
```

```python
import functools

import jax
import jax.numpy as jnp
from jax import lax
from jax.experimental import pallas as pl
from jax.experimental.pallas import tpu as pltpu
from jax.sharding import PartitionSpec as P

MESH = pl.DeviceIdType.MESH
F32 = jnp.float32
BF16 = jnp.bfloat16
I32 = jnp.int32
HALVES = 2
scope = jax.named_scope


def reduce_order(chunks, first, hops):
    link, hop, late = 1.4, 2.6, 1.1
    events = []
    for k in range(chunks):
        t = link * k + (late if k >= first else 0.0)
        if k >= first:
            events.append((1.0 + 0.1 * k, 1, k))
        events += [(t, 2, k), (t + hop, 3, k), (t + hops * hop, 4, k), (t + hops * hop + 3.6, 5, k)]
    return [(stage, k) for _, stage, k in sorted(events)]


def main_kernel(
    nr, nc, relations, tile_cols_n,
    rows_hbm, cols_hbm, count_hbm, vals_hbm, grad_hbm, nodes_hbm, w_hbm,
    dn_ref, ag_ref,
    rows_v, cols_v, count_v, table_v, table_s, chain, gslot, g, w, a, xall, pt,
    nsend, nrecv, ndst, nfin, pbuf, crecv, precv, zbuf, zrecv,
    small_sem, val_sem, load_sem, gs, gr, xs, xr, fs, fr, ns, nrs, nzs, nzr, nfs, nfr,
    cs, cr, ps, pr, zs, zr, zos, zor, aps, apr, acs, acr,
):
    nz = nc // 2
    cap, tile = rows_v.shape[3], chain.shape[2]
    tn, width = gslot.shape[1], gslot.shape[2]
    nd = nodes_hbm.shape[0]
    f = w_hbm.shape[1]
    half = f // HALVES
    tile_rows_n = tn // tile
    lanes_f, lanes_h = f // tile, half // tile
    held_at = tile_rows_n * lanes_h
    plane_rows = pbuf.shape[3]
    chunks = relations * HALVES
    me_r = lax.axis_index("row")
    me_c = lax.axis_index("col")
    z = me_c // 2
    core = me_c % 2
    sibling = {"col": z * 2 + 1 - core}
    lead = core == 1
    other = core == 0

    def row_peer(d):
        return {"row": lax.rem(me_r + d, nr)}

    def z_at(k):
        return {"col": k * 2 + core}

    def z_peer(d):
        return z_at(lax.rem(z + d, nz))

    left_side = z < nz // 2
    inward = jnp.where(left_side, z + 1, z - 1)
    outward = jnp.where(left_side, z - 1, z + 1)
    has_outer = (z > 0) & (z < nz - 1)
    inner = (z == nz // 2 - 1) | (z == nz // 2)
    last_hop = jnp.where(inner, 1, 0)
    passes = jnp.where(has_outer, 1, 0)

    def remote(src, dst, send, recv, dev):
        return pltpu.make_async_remote_copy(
            src_ref=src, dst_ref=dst, send_sem=send, recv_sem=recv, device_id=dev, device_id_type=MESH
        )

    def x_slot(h, k):
        return xall.at[h, pl.ds(pl.multiple_of(k * nd, nd), nd), :]

    def x_from(d):
        return lax.rem(z + nz - d, nz) * 2 + core

    def begin(copies):
        for c in copies:
            c.start()

    with scope("entry"):
        barrier = pltpu.get_barrier_semaphore()
        for d in range(1, nr):
            pl.semaphore_signal(barrier, inc=1, device_id=row_peer(d), device_id_type=MESH)
        for d in range(1, nz):
            pl.semaphore_signal(barrier, inc=1, device_id=z_peer(d), device_id_type=MESH)
        pl.semaphore_signal(barrier, inc=1, device_id=sibling, device_id_type=MESH)

        small = [
            pltpu.make_async_copy(rows_hbm, rows_v, small_sem.at[0]),
            pltpu.make_async_copy(cols_hbm, cols_v, small_sem.at[1]),
            pltpu.make_async_copy(count_hbm, count_v, small_sem.at[2]),
        ]
        load_g = pltpu.make_async_copy(grad_hbm, gslot.at[me_r], load_sem.at[0])
        load_x = [
            pltpu.make_async_copy(nodes_hbm.at[:, h * half : (h + 1) * half], x_slot(h, me_c), load_sem.at[2 + h])
            for h in range(HALVES)
        ]
        load_w = pltpu.make_async_copy(w_hbm, w, load_sem.at[1])
        load_vals = pltpu.make_async_copy(vals_hbm, nsend.at[0 : vals_hbm.shape[0]], val_sem.at[0])
        load_g.start()
        begin(load_x)
        begin(small)
        load_vals.start()
        load_w.start()

    with scope("tables"):
        for c in small:
            c.wait()
        spread = table_v.shape[1]
        slot_lane = lax.broadcasted_iota(I32, (1, cap), 1)
        slot_row = lax.broadcasted_iota(I32, (cap, cap), 0)
        slot_col = lax.broadcasted_iota(I32, (cap, cap), 1)
        place_row = lax.broadcasted_iota(I32, (cap, spread), 0)
        place_col = lax.broadcasted_iota(I32, (cap, spread), 1)
        for r in range(relations):
            key = rows_v[r, 0] * tile_cols_n + cols_v[r, 0]
            key = jnp.where(slot_lane < count_v[0:1, r : r + 1], key, -1)
            down = jnp.max(jnp.where(slot_row == slot_col, jnp.broadcast_to(key, (cap, cap)), -1), axis=1, keepdims=True)
            same = (down == key) & (slot_row < slot_col)
            before = jnp.max(jnp.where(same, slot_row + 1, 0), axis=0, keepdims=True)
            last = jnp.max(jnp.where(down == place_col, place_row + 1, 0), axis=0, keepdims=True)
            table_v[r : r + 1, 0:cap] = before
            table_v[relations + r : relations + r + 1, :] = last
        load_table = pltpu.make_async_copy(table_v, table_s, small_sem.at[3])
        load_table.start()

    with scope("barrier"):
        pl.semaphore_wait(barrier, nr - 1 + nz - 1 + 1)
        load_g.wait()
    with scope("sends"):
        mine = gslot.at[me_r]
        begin([remote(mine, mine, gs.at[0], gr.at[0], row_peer(d)) for d in range(1, nr)])
        for h in range(HALVES):
            load_x[h].wait()
            own = x_slot(h, me_c)
            begin([remote(own, own, xs.at[0], xr.at[h, d - 1], z_peer(d)) for d in range(1, nz)])
            remote(own, own, fs.at[0], fr.at[h, 0], sibling).start()

    with scope("chain"):
        load_table.wait()
        load_vals.wait()
        for r in range(relations):
            chain[r, 0] = jnp.zeros((tile, tile), F32)

        def link(s, carry):
            for r in range(relations):
                t = r * cap + s
                rows = pl.ds(pl.multiple_of(t % lanes_f * tile, tile), tile)
                chain[r, s + 1] = chain[r, table_s[r, s]] + nsend[t // lanes_f, rows, :].astype(F32)
            return carry

        lax.fori_loop(0, cap, link, 0)

    with scope("place"):

        def place(i, carry):
            def one(j, inner):
                for r in range(relations):
                    rows = pl.ds(pl.multiple_of(r * tn + i * tile, tile), tile)
                    cols = pl.ds(pl.multiple_of(j * tile, tile), tile)
                    a[rows, cols] = chain[r, table_s[relations + r, i * tile_cols_n + j]].astype(BF16)
                return inner

            return lax.fori_loop(0, tile_cols_n, one, carry)

        lax.fori_loop(0, tile_rows_n, place, 0)

    def forward(h, d):
        with scope(f"f{h}{d}" if isinstance(d, int) else f"f{h}"):
            slot = x_slot(h, x_from(d))
            remote(slot, slot, xs.at[0], xr.at[h, d - 1], sibling).wait_recv()
            remote(slot, slot, fs.at[0], fr.at[h, d], sibling).start()

    segments = max(tn // f, 1)
    seg = tn // segments

    def y_block(h, d):
        with scope(f"y{h}{d}"):
            slot = x_slot(h, me_c)
            remote(slot, slot, fs.at[0], fr.at[h, d], sibling).wait_recv()
            both = pl.ds(pl.multiple_of(lax.rem(z + nz - d, nz) * 2 * nd, 2 * nd), 2 * nd)
            for r in range(relations):
                part = jnp.dot(a[r * tn : (r + 1) * tn, both], xall[h, both, :], preferred_element_type=F32)
                for i in range(tile_rows_n):
                    for j in range(lanes_h):
                        b = part[i * tile : (i + 1) * tile, j * tile : (j + 1) * tile]
                        at = i * lanes_h + j
                        if d > 0:
                            b = b + chain[r, at]
                        if d < nz - 1:
                            chain[r, at] = b
                        else:
                            top = (i * tile // seg) * half + j * tile
                            side = (i * tile) % seg
                            w[r, top : top + tile, side : side + tile] = b.astype(BF16).T

    def c_copy(k):
        r, h = k % relations, k // relations
        return remote(pbuf.at[r, h], crecv.at[r, h], cs.at[0], cr.at[k], sibling)

    def held_rows(r, h, q):
        first = h * half + q * plane_rows
        block, off = first // tile, first % tile
        assert off + plane_rows <= tile
        return jnp.concatenate(
            [chain[r, held_at + block * lanes_f + j, off : off + plane_rows, :] for j in range(lanes_f)], axis=1
        )

    def terms(k):
        r, h = k % relations, k // relations
        with scope(f"terms{k}"):
            v = jnp.dot(w[r, 0:half, 0:seg], g[0:seg, :], preferred_element_type=F32)
            for s in range(1, segments):
                v = v + jnp.dot(
                    w[r, s * half : (s + 1) * half, 0:seg], g[s * seg : (s + 1) * seg, :], preferred_element_type=F32
                )
            for i in range(lanes_h):
                for j in range(lanes_f):
                    at = held_at + (h * lanes_h + i) * lanes_f + j
                    chain[r, at] = v[i * tile : (i + 1) * tile, j * tile : (j + 1) * tile]

            @pl.when(other)
            def _():
                for q in range(nr):
                    pbuf[r, h, q] = held_rows(r, h, q).astype(BF16)
                c_copy(k).start()

    def plane_scatter(k):
        r, h = k % relations, k // relations
        with scope(f"s1{k}"):
            c_copy(k).wait_recv()
            for q in range(nr):
                pbuf[r, h, q] = (held_rows(r, h, q) + crecv[r, h, q].astype(F32)).astype(BF16)
            begin([
                remote(pbuf.at[r, h, lax.rem(me_r + d, nr)], precv.at[k, d - 1], ps.at[0], pr.at[k], row_peer(d))
                for d in range(1, nr)
            ])

    def pa_copies(k):
        part = ag_ref.at[k % relations, k // relations, me_r]
        return [remote(part, part, aps.at[0], apr.at[k, d - 1], row_peer(d)) for d in range(1, nr)]

    def ca_copy(k, d):
        part = ag_ref.at[k % relations, k // relations, lax.rem(me_r + nr - d, nr)]
        return remote(part, part, acs.at[0], acr.at[0], sibling)

    def z_in(k, held):
        remote(zbuf.at[k, held], zrecv.at[k, last_hop], zs.at[0], zr.at[k, last_hop], z_at(inward)).start()

    def z_came(k, slot):
        remote(zrecv.at[k, slot], zrecv.at[k, slot], zs.at[0], zr.at[k, slot], sibling).wait_recv()

    def z_out(k):
        part = ag_ref.at[k % relations, k // relations, me_r]
        return remote(part, part, zos.at[0], zor.at[k], z_at(outward))

    def plane_sum(k):
        r, h = k % relations, k // relations
        remote(precv.at[k], precv.at[k], ps.at[0], pr.at[k], sibling).wait_recv()
        part = pbuf[r, h, me_r].astype(F32)
        for d in range(1, nr):
            part = part + precv[k, d - 1].astype(F32)
        zbuf[k, 0] = part.astype(BF16)

        @pl.when(jnp.logical_not(has_outer))
        def _():
            z_in(k, 0)

    def z_sum(k):
        @pl.when(has_outer)
        def _():
            z_came(k, 0)
            zbuf[k, 1] = (zbuf[k, 0].astype(F32) + zrecv[k, 0].astype(F32)).astype(BF16)
            z_in(k, 1)

    def plane_gather(k):
        @pl.when(inner)
        def _():
            z_came(k, 1)
            total = zbuf[k, passes].astype(F32) + zrecv[k, 1].astype(F32)
            ag_ref[k % relations, k // relations, me_r] = total.astype(BF16)

        @pl.when(jnp.logical_not(inner))
        def _():
            z_out(k).wait_recv()

        @pl.when(has_outer)
        def _():
            z_out(k).start()

        begin(pa_copies(k))
        ca_copy(k, 0).start()

    def core_gather(k):
        copies = pa_copies(k)
        for d in range(1, nr):
            copies[d - 1].wait_recv()
            ca_copy(k, d).start()

    def mix(k, carry):
        cols = pl.ds(pl.multiple_of(k * 2 * nd, 2 * nd), 2 * nd)
        both = jnp.dot(pt[...], a[:, cols], preferred_element_type=F32)
        nsend[k * 2] = both[:, :nd].astype(BF16)
        nsend[k * 2 + 1] = both[:, nd:].astype(BF16)
        return carry

    def n_core(part):
        span = slice(part * nz, (part + 1) * nz)
        return remote(nsend.at[span], nrecv.at[span], ns.at[0], nrs.at[part], sibling)

    def dn_send(k, p, slot, to):
        remote(nsend.at[k * 2 + p], ndst.at[slot, p], nzs.at[0], nzr.at[slot, p], z_at(to)).start()

    def dn_arrived(slot, p):
        came = ndst.at[slot, p]
        remote(came, came, nzs.at[0], nzr.at[slot, p], sibling).wait_recv()

    def dn_total(k, p):
        return nsend[k * 2 + p].astype(F32) + nrecv[k * 2 + p].astype(F32)

    def dn_first():
        for part in range(2):
            n_core(part).wait_recv()
        for j in range(nz - 1):
            up, down = nz - 1 - j, j
            for p in range(2):

                @pl.when(z == 0)
                def _():
                    nsend[up * 2 + p] = dn_total(up, p).astype(BF16)
                    dn_send(up, p, up + 1, 1)

                @pl.when(z == nz - 1)
                def _():
                    nsend[down * 2 + p] = dn_total(down, p).astype(BF16)
                    dn_send(down, p, down, nz - 2)

    def dn_pass(k, p, slot, to):
        dn_arrived(slot, p)
        nsend[k * 2 + p] = (dn_total(k, p) + ndst[slot, p].astype(F32)).astype(BF16)
        dn_send(k, p, slot, to)

    def dn_rest():
        for j in range(nz - 1):
            up, down = nz - 1 - j, j
            for p in range(2):

                @pl.when((z > 0) & (z < up))
                def _():
                    dn_pass(up, p, up + 1, z + 1)

                @pl.when((z > down) & (z < nz - 1))
                def _():
                    dn_pass(down, p, down, z - 1)

    own_dn = lambda: remote(nfin, dn_ref, nfs.at[0], nfr.at[0], sibling)

    def on_lead(*work):
        @pl.when(lead)
        def _():
            for w in work:
                w()

    def serve(*ks):
        on_lead(*[functools.partial(plane_scatter, k) for k in ks])

    y_block(0, 0)
    if nz > 1:
        forward(0, 1)
        y_block(0, 1)
    with scope("waitg"):
        load_w.wait()
        slots = gslot.at[0 : nr - 1]
        remote(slots, slots, gs.at[0], gr.at[0], sibling).wait_recv()
    with scope("premix"):
        for k in range(nr):
            g[:, k * width : (k + 1) * width] = gslot[k]
        for r in range(relations):
            pt[:, r * tn : (r + 1) * tn] = lax.dot_general(
                w[r], g[...], (((1,), (1,)), ((), ())), preferred_element_type=F32
            ).astype(BF16)

    def mix_step(k, carry):
        mix(k, carry)

        @pl.when(k < nz - 2)
        def _():
            forward(0, k + 2)

        @pl.when(lead & (k == nz // 2 - 1))
        def _():
            n_core(0).start()

        return carry

    with scope("mix"):
        lax.fori_loop(0, nz, mix_step, 0)
    on_lead(lambda: n_core(1).start())
    for d in range(2, nz):
        y_block(0, d)

    @pl.when(other)
    def _():
        with scope("dn_first"):
            dn_first()

    for k in range(relations):
        terms(k)
    for d in range(nz):
        if d > 0:
            forward(1, d)
            y_block(1, d - 1)
        if 0 < d <= relations:
            serve(d - 1)
    for d in range(nz, relations + 1):
        serve(d - 1)
    y_block(1, nz - 1)
    for k in range(relations, chunks):
        terms(k)

    stages = {1: plane_scatter, 2: plane_sum, 3: z_sum, 4: plane_gather, 5: core_gather}

    def reduce_all(hops):
        for stage, k in reduce_order(chunks, relations, hops):
            with scope(f"s{stage}_{k}"):
                stages[stage](k)

    @pl.when(lead & inner)
    def _():
        reduce_all(nz // 2)

    @pl.when(lead & jnp.logical_not(inner))
    def _():
        reduce_all(nz - 1)

    @pl.when(lead)
    def _():
        with scope("end"):
            own_dn().wait_recv()
            sent = nsend.at[0 : nz * 2]
            for ref, sem in ((sent, ns), (precv, ps), (zbuf.at[:, 0], zs), (precv, aps), (ag_ref, acs)):
                remote(ref, ref, sem.at[0], sem.at[0], sibling).wait_send()

            @pl.when(has_outer)
            def _():
                remote(zbuf.at[:, 0], zbuf.at[:, 0], zos.at[0], zos.at[0], sibling).wait_send()

    @pl.when(other)
    def _():
        with scope("dn_rest"):
            dn_rest()
        with scope("dn_fin"):
            for p in range(2):

                @pl.when(z > 0)
                def _():
                    dn_arrived(z + 1, p)

                @pl.when(z < nz - 1)
                def _():
                    dn_arrived(z, p)

                own = nsend[z * 2 + p].astype(F32) + nrecv[z * 2 + p].astype(F32)
                below = jnp.where(z > 0, ndst[z + 1, p].astype(F32), 0.0)
                above = jnp.where(z < nz - 1, ndst[z, p].astype(F32), 0.0)
                done = (own + below + above).T.astype(BF16)
                if p == 0:
                    dn_ref[...] = done
                else:
                    nfin[...] = done
            own_dn().start()
        with scope("oend"):
            remote(ag_ref, ag_ref, acs.at[0], acr.at[0], sibling).wait_recv()
            sent = nsend.at[0 : (nz - 1) * 2]
            for ref, sem in ((pbuf, cs), (sent, nzs), (nfin, nfs)):
                remote(ref, ref, sem.at[0], sem.at[0], sibling).wait_send()

    sent_x = xall.at[:, 0 : (nz - 1) * nd, :]
    sent_f = xall.at[:, 0 : nz * nd, :]
    for ref, sem in ((gslot.at[0 : nr - 1], gs), (sent_x, xs), (sent_f, fs)):
        remote(ref, ref, sem.at[0], sem.at[0], sibling).wait_send()


def widen_kernel(dn_ref, dw_ref, dn_out, dw_out, wide, out_sem):
    parts, rows = wide.shape[0], wide.shape[1]
    stores = [
        pltpu.make_async_copy(wide.at[k], dw_out.at[k * rows : (k + 1) * rows, :], out_sem.at[k])
        for k in range(parts)
    ]
    stores.append(pltpu.make_async_copy(dn_ref, dn_out, out_sem.at[parts]))
    stores[parts].start()
    for k in range(parts):
        wide[k] = dw_ref[k * rows : (k + 1) * rows, :].astype(F32)
        stores[k].start()
    for c in stores:
        c.wait()


def widen(d_nodes, gathered):
    total, f = gathered.shape
    parts = 6 if total % 96 == 0 else 1
    rows = total // parts
    hbm = pl.BlockSpec(memory_space=pltpu.HBM)
    vmem = pl.BlockSpec(memory_space=pltpu.VMEM)
    return pl.pallas_call(
        widen_kernel,
        in_specs=[vmem, vmem],
        out_specs=(hbm, hbm),
        out_shape=(
            jax.ShapeDtypeStruct(d_nodes.shape, BF16),
            jax.ShapeDtypeStruct(gathered.shape, F32),
        ),
        scratch_shapes=[
            pltpu.VMEM((parts, rows, f), F32),
            pltpu.SemaphoreType.DMA((parts + 1,)),
        ],
    )(
        pltpu.with_memory_space_constraint(d_nodes, pltpu.VMEM),
        pltpu.with_memory_space_constraint(gathered, pltpu.VMEM),
    )


def body(nr, nc, out_grad, node_in, weights, tile_vals, tile_rows, tile_cols, tile_count):
    relations, f = weights.shape[0], weights.shape[1]
    cap, tile = tile_vals.shape[3], tile_vals.shape[4]
    tn, width = out_grad.shape
    nd = node_in.shape[0]
    sn = nd * nc
    nz = nc // 2
    half = f // HALVES
    plane_rows = half // nr
    chunks = relations * HALVES
    assert nz % 2 == 0
    places = (tn // tile) * (sn // tile)
    spread = -(-max(places, cap) // 128) * 128
    blocks = max(cap + 1, (tn // tile) * (half // tile) + (f // tile) ** 2)
    slots = relations * cap * tile // f
    assert nd == tile and slots * f == relations * cap * tile
    dma = lambda *n: pltpu.SemaphoreType.DMA(n)
    hbm = pl.BlockSpec(memory_space=pltpu.HBM)
    vmem = pl.BlockSpec(memory_space=pltpu.VMEM)
    d_nodes, gathered = pl.pallas_call(
        functools.partial(main_kernel, nr, nc, relations, sn // tile),
        out_shape=(
            pltpu.VMEM((nd, f), BF16),
            pltpu.VMEM((relations, HALVES, nr, plane_rows, f), BF16),
        ),
        in_specs=[hbm] * 7,
        out_specs=(vmem, vmem),
        scratch_shapes=[
            pltpu.VMEM(tile_rows.shape, I32),
            pltpu.VMEM(tile_cols.shape, I32),
            pltpu.VMEM((1, relations), I32),
            pltpu.VMEM((-(-2 * relations // 8) * 8, spread), I32),
            pltpu.SMEM((-(-2 * relations // 8) * 8, spread), I32),
            pltpu.VMEM((relations, blocks, tile, tile), F32),
            pltpu.VMEM((nr, tn, width), BF16),
            pltpu.VMEM((tn, f), BF16),
            pltpu.VMEM(weights.shape, BF16),
            pltpu.VMEM((relations * tn, sn), BF16),
            pltpu.VMEM((HALVES, sn, half), BF16),
            pltpu.VMEM((f, relations * tn), BF16),
            pltpu.VMEM((max(nz * 2, slots), f, nd), BF16),
            pltpu.VMEM((nz * 2, f, nd), BF16),
            pltpu.VMEM((nz + 1, 2, f, nd), BF16),
            pltpu.VMEM((nd, f), BF16),
            pltpu.VMEM((relations, HALVES, nr, plane_rows, f), BF16),
            pltpu.VMEM((relations, HALVES, nr, plane_rows, f), BF16),
            pltpu.VMEM((chunks, nr - 1, plane_rows, f), BF16),
            pltpu.VMEM((chunks, 2, plane_rows, f), BF16),
            pltpu.VMEM((chunks, 2, plane_rows, f), BF16),
            dma(4), dma(1), dma(2 + HALVES),
            dma(1), dma(1),
            dma(1), dma(HALVES, nz - 1),
            dma(1), dma(HALVES, nz),
            dma(1), dma(2),
            dma(1), dma(nz + 1, 2),
            dma(1), dma(1),
            dma(1), dma(chunks),
            dma(1), dma(chunks),
            dma(1), dma(chunks, 2),
            dma(1), dma(chunks),
            dma(1), dma(chunks, nr - 1),
            dma(1), dma(1),
        ],
        compiler_params=pltpu.CompilerParams(
            collective_id=0, has_side_effects=True, vmem_limit_bytes=63000 * 1024
        ),
    )(
        tile_rows,
        tile_cols,
        tile_count.reshape(1, relations),
        tile_vals.reshape(slots, f, tile),
        out_grad,
        node_in,
        weights,
    )
    d_nodes, d_weights = widen(d_nodes, gathered.reshape(relations * f, f))
    return d_nodes, d_weights.reshape(relations, f, f)


def solution(mesh):
    return jax.shard_map(
        functools.partial(body, mesh.shape["row"], mesh.shape["col"]),
        mesh=mesh,
        in_specs=(
            P("col", "row"),
            P(("row", "col"), None),
            P(),
            P(None, "col", "row", None, None, None),
            P(None, "col", "row", None),
            P(None, "col", "row", None),
            P(None, "col", "row"),
        ),
        out_specs=(P(("row", "col"), None), P()),
        check_vma=False,
    )
```

```python
import functools

import jax
import jax.numpy as jnp
from jax import lax
from jax.experimental import pallas as pl
from jax.experimental.pallas import tpu as pltpu
from jax.sharding import PartitionSpec as P

MESH = pl.DeviceIdType.MESH
F32 = jnp.float32
BF16 = jnp.bfloat16
I32 = jnp.int32
HALVES = 2
WIDE = 1
scope = jax.named_scope


def reduce_order(chunks, first, half_line, wide):
    link, hop, late = 1.4, 3.6, 0.3
    events = []
    for k in range(chunks):
        t = link * k + (late if k >= first else 0.0)
        if k >= first:
            events.append((0.5 + 0.1 * k, 1, k))
        if k > 0:
            events.append((t, 2, k))
        met = t + half_line * hop + 0.4
        out = 0.3 if k < wide else (half_line - 1) * 2.8
        events += [(t + hop, 3, k), (met, 4, k), (met + out, 5, k), (met + 9.0, 6, k)]
    return [(stage, k) for _, stage, k in sorted(events)]


def main_kernel(
    nr, nc, relations, tile_cols_n,
    rows_hbm, cols_hbm, count_hbm, vals_hbm, grad_hbm, nodes_hbm, w_hbm,
    dn_ref, ag_ref,
    rows_v, cols_v, count_v, table_v, table_s, chain, gslot, g, w, a, xall, pt,
    nsend, nrecv, ndst, nfin, pbuf, crecv, precv, zbuf, zrecv,
    small_sem, val_sem, load_sem, gs, gr, xs, xr, fs, fr, ns, nrs, nzs, nzr, nfs, nfr,
    cs, cr, ps, pr, zs, zr, aps, apr, acs, acr,
):
    nz = nc // 2
    cap, tile = rows_v.shape[3], chain.shape[2]
    tn, width = gslot.shape[1], gslot.shape[2]
    nd = nodes_hbm.shape[0]
    f = w_hbm.shape[1]
    half = f // HALVES
    tile_rows_n = tn // tile
    lanes_f, lanes_h = f // tile, half // tile
    held_at = tile_rows_n * lanes_h
    plane_rows = pbuf.shape[3]
    chunks = relations * HALVES
    me_r = lax.axis_index("row")
    me_c = lax.axis_index("col")
    z = me_c // 2
    core = me_c % 2
    sibling = {"col": z * 2 + 1 - core}
    lead = core == 1
    other = core == 0

    def row_at(d):
        at, bit = me_r, 1
        while bit < nr:
            if d & bit:
                at = at + bit - 2 * bit * lax.rem(at // bit, 2)
            bit *= 2
        return at

    def row_peer(d):
        return {"row": row_at(d)}

    def z_at(k):
        return {"col": k * 2 + core}

    def z_peer(d):
        return z_at(lax.rem(z + d, nz))

    left_side = z < nz // 2
    inward = jnp.where(left_side, z + 1, z - 1)
    has_outer = (z > 0) & (z < nz - 1)
    inner = (z == nz // 2 - 1) | (z == nz // 2)
    side = jnp.where(left_side, 1, 2)
    outward = jnp.where(left_side, z - 1, z + 1)
    wide = min(WIDE, chunks)

    def remote(src, dst, send, recv, dev):
        return pltpu.make_async_remote_copy(
            src_ref=src, dst_ref=dst, send_sem=send, recv_sem=recv, device_id=dev, device_id_type=MESH
        )

    def x_slot(h, k):
        return xall.at[h, pl.ds(pl.multiple_of(k * nd, nd), nd), :]

    def x_from(d):
        return lax.rem(z + nz - d, nz) * 2 + core

    def begin(copies):
        for c in copies:
            c.start()

    with scope("entry"):
        barrier = pltpu.get_barrier_semaphore()
        for d in range(1, nr):
            pl.semaphore_signal(barrier, inc=1, device_id=row_peer(d), device_id_type=MESH)
        for d in range(1, nz):
            pl.semaphore_signal(barrier, inc=1, device_id=z_peer(d), device_id_type=MESH)
        pl.semaphore_signal(barrier, inc=1, device_id=sibling, device_id_type=MESH)

        small = [
            pltpu.make_async_copy(rows_hbm, rows_v, small_sem.at[0]),
            pltpu.make_async_copy(cols_hbm, cols_v, small_sem.at[1]),
            pltpu.make_async_copy(count_hbm, count_v, small_sem.at[2]),
        ]
        load_g = pltpu.make_async_copy(grad_hbm, gslot.at[me_r], load_sem.at[0])
        load_x = [
            pltpu.make_async_copy(nodes_hbm.at[:, h * half : (h + 1) * half], x_slot(h, me_c), load_sem.at[2 + h])
            for h in range(HALVES)
        ]
        load_w = pltpu.make_async_copy(w_hbm, w, load_sem.at[1])
        load_vals = pltpu.make_async_copy(vals_hbm, nsend.at[0 : vals_hbm.shape[0]], val_sem.at[0])
        load_g.start()
        begin(load_x)
        begin(small)
        load_vals.start()
        load_w.start()

    with scope("tables"):
        for c in small:
            c.wait()
        spread = table_v.shape[1]
        slot_lane = lax.broadcasted_iota(I32, (1, cap), 1)
        slot_row = lax.broadcasted_iota(I32, (cap, cap), 0)
        slot_col = lax.broadcasted_iota(I32, (cap, cap), 1)
        place_row = lax.broadcasted_iota(I32, (cap, spread), 0)
        place_col = lax.broadcasted_iota(I32, (cap, spread), 1)
        for r in range(relations):
            key = rows_v[r, 0] * tile_cols_n + cols_v[r, 0]
            key = jnp.where(slot_lane < count_v[0:1, r : r + 1], key, -1)
            down = jnp.max(jnp.where(slot_row == slot_col, jnp.broadcast_to(key, (cap, cap)), -1), axis=1, keepdims=True)
            same = (down == key) & (slot_row < slot_col)
            before = jnp.max(jnp.where(same, slot_row + 1, 0), axis=0, keepdims=True)
            last = jnp.max(jnp.where(down == place_col, place_row + 1, 0), axis=0, keepdims=True)
            table_v[r : r + 1, 0:cap] = before
            table_v[relations + r : relations + r + 1, :] = last
        load_table = pltpu.make_async_copy(table_v, table_s, small_sem.at[3])
        load_table.start()

    with scope("barrier"):
        pl.semaphore_wait(barrier, nr - 1 + nz - 1 + 1)
        load_g.wait()
    with scope("sends"):
        mine = gslot.at[me_r]
        begin([remote(mine, mine, gs.at[0], gr.at[0], row_peer(d)) for d in range(1, nr)])

        def send_x(h):
            load_x[h].wait()
            own = x_slot(h, me_c)

            begin([remote(own, own, xs.at[0], xr.at[h, d - 1], z_peer(d)) for d in range(1, nz)])
            remote(own, own, fs.at[0], fr.at[h, 0], sibling).start()

        send_x(0)

    with scope("chain"):
        load_table.wait()
        load_vals.wait()
        for r in range(relations):
            chain[r, 0] = jnp.zeros((tile, tile), F32)

        def link(s, carry):
            for r in range(relations):
                t = r * cap + s
                rows = pl.ds(pl.multiple_of(t % lanes_f * tile, tile), tile)
                chain[r, s + 1] = chain[r, table_s[r, s]] + nsend[t // lanes_f, rows, :].astype(F32)
            return carry

        lax.fori_loop(0, cap, link, 0)

    with scope("place"):

        def place(i, carry):
            def one(j, inner):
                for r in range(relations):
                    rows = pl.ds(pl.multiple_of(r * tn + i * tile, tile), tile)
                    cols = pl.ds(pl.multiple_of(j * tile, tile), tile)
                    a[rows, cols] = chain[r, table_s[relations + r, i * tile_cols_n + j]].astype(BF16)
                return inner

            return lax.fori_loop(0, tile_cols_n, one, carry)

        lax.fori_loop(0, tile_rows_n, place, 0)

    def forward(h, d):
        with scope(f"f{h}{d}" if isinstance(d, int) else f"f{h}"):
            slot = x_slot(h, x_from(d))
            remote(slot, slot, xs.at[0], xr.at[h, d - 1], sibling).wait_recv()
            remote(slot, slot, fs.at[0], fr.at[h, d], sibling).start()

    segments = max(tn // f, 1)
    seg = tn // segments

    def y_block(h, d):
        with scope(f"y{h}{d}"):
            slot = x_slot(h, me_c)
            remote(slot, slot, fs.at[0], fr.at[h, d], sibling).wait_recv()
            both = pl.ds(pl.multiple_of(lax.rem(z + nz - d, nz) * 2 * nd, 2 * nd), 2 * nd)
            for r in range(relations):
                part = jnp.dot(a[r * tn : (r + 1) * tn, both], xall[h, both, :], preferred_element_type=F32)
                for i in range(tile_rows_n):
                    for j in range(lanes_h):
                        b = part[i * tile : (i + 1) * tile, j * tile : (j + 1) * tile]
                        at = i * lanes_h + j
                        if d > 0:
                            b = b + chain[r, at]
                        if d < nz - 1:
                            chain[r, at] = b
                        else:
                            top = (i * tile // seg) * half + j * tile
                            side = (i * tile) % seg
                            w[r, top : top + tile, side : side + tile] = b.astype(BF16).T

    def c_copy(k):
        r, h = k % relations, k // relations
        return remote(pbuf.at[r, h], crecv.at[r, h], cs.at[0], cr.at[k], sibling)

    def held_rows(r, h, q):
        first = h * half + q * plane_rows
        block, off = first // tile, first % tile
        assert off + plane_rows <= tile
        return jnp.concatenate(
            [chain[r, held_at + block * lanes_f + j, off : off + plane_rows, :] for j in range(lanes_f)], axis=1
        )

    def terms(k):
        r, h = k % relations, k // relations
        with scope(f"terms{k}"):
            v = jnp.dot(w[r, 0:half, 0:seg], g[0:seg, :], preferred_element_type=F32)
            for s in range(1, segments):
                v = v + jnp.dot(
                    w[r, s * half : (s + 1) * half, 0:seg], g[s * seg : (s + 1) * seg, :], preferred_element_type=F32
                )
            for i in range(lanes_h):
                for j in range(lanes_f):
                    at = held_at + (h * lanes_h + i) * lanes_f + j
                    chain[r, at] = v[i * tile : (i + 1) * tile, j * tile : (j + 1) * tile]

            @pl.when(other)
            def _():
                for q in range(nr):
                    pbuf[r, h, q] = held_rows(r, h, q).astype(BF16)
                c_copy(k).start()

    def plane_scatter(r, h):
        k = h * relations + r
        with scope(f"s1_h{h}"):
            remote(pbuf.at[r, h], crecv.at[r, h], cs.at[0], cr.at[k], sibling).wait_recv()
            for q in range(nr):
                pbuf[r, h, q] = (held_rows(r, h, q) + crecv[r, h, q].astype(F32)).astype(BF16)
            begin([
                remote(pbuf.at[r, h, row_at(d)], precv.at[k, d - 1], ps.at[0], pr.at[k], row_peer(d))
                for d in range(1, nr)
            ])

    def pa_copies(k):
        part = ag_ref.at[k % relations, k // relations, me_r]
        return [remote(part, part, aps.at[0], apr.at[k, d - 1], row_peer(d)) for d in range(1, nr)]

    def ca_copy(k, d):
        part = ag_ref.at[k % relations, k // relations, row_at(d)]
        return remote(part, part, acs.at[0], acr.at[0], sibling)

    def z_hand(k, held):
        sent = zbuf.at[k, held]

        @pl.when(inner)
        def _():
            if k < wide:
                for d in range(1, nz):
                    remote(sent, zrecv.at[k, side], zs.at[d - 1], zr.at[k, side], z_peer(d)).start()
            else:
                remote(sent, zrecv.at[k, side], zs.at[0], zr.at[k, side], z_at(inward)).start()

        @pl.when(jnp.logical_not(inner))
        def _():
            remote(sent, zrecv.at[k, 0], zs.at[0], zr.at[k, 0], z_at(inward)).start()

    def z_came(k, slot):
        remote(zrecv.at[k, slot], zrecv.at[k, slot], zs.at[0], zr.at[k, slot], sibling).wait_recv()

    def plane_sum(k):
        r, h = k % relations, k // relations
        remote(precv.at[k], precv.at[k], ps.at[0], pr.at[k], sibling).wait_recv()
        part = pbuf[r, h, me_r].astype(F32)
        for d in range(1, nr):
            part = part + precv[k, d - 1].astype(F32)
        zbuf[k, 0] = part.astype(BF16)

        @pl.when(jnp.logical_not(has_outer))
        def _():
            z_hand(k, 0)

    def z_sum(k):
        @pl.when(has_outer)
        def _():
            z_came(k, 0)
            zbuf[k, 1] = (zbuf[k, 0].astype(F32) + zrecv[k, 0].astype(F32)).astype(BF16)
            z_hand(k, 1)

    def z_out(k):
        part = ag_ref.at[k % relations, k // relations, me_r]
        return remote(part, part, zs.at[1], zr.at[k, 1], z_at(outward))

    def gather_on(k):
        begin(pa_copies(k))
        ca_copy(k, 0).start()

    def inner_gather(k):
        @pl.when(inner)
        def _():
            z_came(k, 3 - side)
            own = zbuf[k, jnp.where(has_outer, 1, 0)].astype(F32)
            ag_ref[k % relations, k // relations, me_r] = (own + zrecv[k, 3 - side].astype(F32)).astype(BF16)
            if k >= wide:
                pl.when(has_outer)(lambda: z_out(k).start())
            gather_on(k)

    def outer_gather(k):
        @pl.when(jnp.logical_not(inner))
        def _():
            if k < wide:
                z_came(k, 1)
                z_came(k, 2)
                both = zrecv[k, 1].astype(F32) + zrecv[k, 2].astype(F32)
                ag_ref[k % relations, k // relations, me_r] = both.astype(BF16)
            else:
                z_out(k).wait_recv()
                pl.when(has_outer)(lambda: z_out(k).start())
            gather_on(k)

    def core_gather(k):
        copies = pa_copies(k)
        for d in range(1, nr):
            copies[d - 1].wait_recv()
            ca_copy(k, d).start()

    def mix(k, carry):
        cols = pl.ds(pl.multiple_of(k * 2 * nd, 2 * nd), 2 * nd)
        both = jnp.dot(pt[...], a[:, cols], preferred_element_type=F32)
        nsend[k * 2] = both[:, :nd].astype(BF16)
        nsend[k * 2 + 1] = both[:, nd:].astype(BF16)
        return carry

    def n_core(k):
        span = pl.ds(2 * k, 2)
        return remote(nsend.at[span], nrecv.at[span], ns.at[0], nrs.at[k], sibling)

    def dn_send(k, p, slot, to):
        remote(nsend.at[k * 2 + p], ndst.at[slot, p], nzs.at[0], nzr.at[slot, p], z_at(to)).start()

    def dn_arrived(slot, p):
        came = ndst.at[slot, p]
        remote(came, came, nzs.at[0], nzr.at[slot, p], sibling).wait_recv()

    def dn_total(k, p):
        return nsend[k * 2 + p].astype(F32) + nrecv[k * 2 + p].astype(F32)

    def dn_first():
        for k in range(nz):
            n_core(k).wait_recv()
        for j in range(nz - 1):
            up, down = nz - 1 - j, j
            for p in range(2):

                @pl.when(z == 0)
                def _():
                    nsend[up * 2 + p] = dn_total(up, p).astype(BF16)
                    dn_send(up, p, up + 1, 1)

                @pl.when(z == nz - 1)
                def _():
                    nsend[down * 2 + p] = dn_total(down, p).astype(BF16)
                    dn_send(down, p, down, nz - 2)

    def dn_pass(k, p, slot, to):
        dn_arrived(slot, p)
        nsend[k * 2 + p] = (dn_total(k, p) + ndst[slot, p].astype(F32)).astype(BF16)
        dn_send(k, p, slot, to)

    def dn_up():
        def step(m, carry):
            up, p = nz - 1 - m // 2, m % 2

            @pl.when((z > 0) & (z < up))
            def _():
                dn_pass(up, p, up + 1, z + 1)

            return carry

        lax.fori_loop(0, 2 * (nz - 1), step, 0)

    def dn_down():
        def step(m, carry):
            down, p = m // 2, m % 2

            @pl.when((z > down) & (z < nz - 1))
            def _():
                dn_pass(down, p, down, z - 1)

            return carry

        lax.fori_loop(0, 2 * (nz - 1), step, 0)

    def dn_rest():
        @pl.when(left_side)
        def _():
            dn_up()
            dn_down()

        @pl.when(jnp.logical_not(left_side))
        def _():
            dn_down()
            dn_up()

    own_dn = lambda: remote(nfin, dn_ref, nfs.at[0], nfr.at[0], sibling)

    y_block(0, 0)
    if nz > 1:
        forward(0, 1)
        y_block(0, 1)
    for h in range(1, HALVES):
        with scope("sends1"):
            send_x(h)
    with scope("waitg"):
        load_w.wait()
        slots = gslot.at[0 : nr - 1]
        remote(slots, slots, gs.at[0], gr.at[0], sibling).wait_recv()
    with scope("premix"):
        for k in range(nr):
            g[:, k * width : (k + 1) * width] = gslot[k]
        for r in range(relations):
            pt[:, r * tn : (r + 1) * tn] = lax.dot_general(
                w[r], g[...], (((1,), (1,)), ((), ())), preferred_element_type=F32
            ).astype(BF16)

    def lead_mix(k, carry):
        mix(k, carry)
        n_core(k).start()
        return carry

    def other_mix(k, carry):
        mix(k, carry)

        @pl.when(k > 0)
        def _():
            forward(1, k)

        return carry

    for d in range(2, nz):
        forward(0, d)

    @pl.when(lead)
    def _():
        with scope("mix"):
            lax.fori_loop(0, nz, lead_mix, 0)

    for d in range(2, nz):
        y_block(0, d)
    for k in range(relations):
        terms(k)

        @pl.when(lead)
        def _():
            plane_scatter(k, 0)

    @pl.when(lead)
    def _():
        for d in range(1, nz):
            forward(1, d)

    @pl.when(other)
    def _():
        with scope("mix"):
            lax.fori_loop(0, nz, other_mix, 0)
        with scope("dn_first"):
            dn_first()

    for d in range(nz):
        y_block(1, d)

    @pl.when(lead)
    def _():
        with scope("s2_0"):
            plane_sum(0)

    for k in range(relations, chunks):
        terms(k)

    stages = {
        1: lambda k: plane_scatter(k - relations, 1),
        2: plane_sum,
        3: z_sum,
        4: inner_gather,
        5: outer_gather,
        6: core_gather,
    }

    @pl.when(lead)
    def _():
        for stage, k in reduce_order(chunks, relations, nz // 2, wide):
            with scope(f"s{stage}_{k}"):
                stages[stage](k)
        with scope("end"):
            own_dn().wait_recv()
            sent = nsend.at[0 : nz * 2]
            for ref, sem in ((sent, ns), (precv, ps), (zbuf.at[:, 0], zs), (precv, aps), (ag_ref, acs)):
                remote(ref, ref, sem.at[0], sem.at[0], sibling).wait_send()

            def z_left(count, at):
                if count > 0:
                    ref = zbuf.at[0:count, 0]
                    remote(ref, ref, zs.at[at], zs.at[at], sibling).wait_send()

            @pl.when(has_outer)
            def _():
                z_left(chunks - wide, 1)

            @pl.when(inner)
            def _():
                for d in range(2, nz):
                    z_left(wide, d - 1)

    @pl.when(other)
    def _():
        with scope("dn_rest"):
            dn_rest()
        with scope("dn_fin"):
            for p in range(2):

                @pl.when(z > 0)
                def _():
                    dn_arrived(z + 1, p)

                @pl.when(z < nz - 1)
                def _():
                    dn_arrived(z, p)

                own = nsend[z * 2 + p].astype(F32) + nrecv[z * 2 + p].astype(F32)
                below = jnp.where(z > 0, ndst[z + 1, p].astype(F32), 0.0)
                above = jnp.where(z < nz - 1, ndst[z, p].astype(F32), 0.0)
                done = (own + below + above).T.astype(BF16)
                if p == 0:
                    dn_ref[...] = done
                else:
                    nfin[...] = done
            own_dn().start()
        with scope("oend"):
            remote(ag_ref, ag_ref, acs.at[0], acr.at[0], sibling).wait_recv()
            sent = nsend.at[0 : (nz - 1) * 2]
            for ref, sem in ((pbuf, cs), (sent, nzs), (nfin, nfs)):
                remote(ref, ref, sem.at[0], sem.at[0], sibling).wait_send()

    sent_x = xall.at[:, 0 : (nz - 1) * nd, :]
    sent_f = xall.at[:, 0 : nz * nd, :]
    for ref, sem in ((gslot.at[0 : nr - 1], gs), (sent_x, xs), (sent_f, fs)):
        remote(ref, ref, sem.at[0], sem.at[0], sibling).wait_send()


def widen_kernel(dn_ref, dw_ref, dn_out, dw_out, wide, out_sem):
    parts, rows = wide.shape[0], wide.shape[1]
    stores = [
        pltpu.make_async_copy(wide.at[k], dw_out.at[k * rows : (k + 1) * rows, :], out_sem.at[k])
        for k in range(parts)
    ]
    stores.append(pltpu.make_async_copy(dn_ref, dn_out, out_sem.at[parts]))
    stores[parts].start()
    for k in range(parts):
        wide[k] = dw_ref[k * rows : (k + 1) * rows, :].astype(F32)
        stores[k].start()
    for c in stores:
        c.wait()


def widen(d_nodes, gathered):
    total, f = gathered.shape
    parts = 6 if total % 96 == 0 else 1
    rows = total // parts
    hbm = pl.BlockSpec(memory_space=pltpu.HBM)
    vmem = pl.BlockSpec(memory_space=pltpu.VMEM)
    return pl.pallas_call(
        widen_kernel,
        in_specs=[vmem, vmem],
        out_specs=(hbm, hbm),
        out_shape=(
            jax.ShapeDtypeStruct(d_nodes.shape, BF16),
            jax.ShapeDtypeStruct(gathered.shape, F32),
        ),
        scratch_shapes=[
            pltpu.VMEM((parts, rows, f), F32),
            pltpu.SemaphoreType.DMA((parts + 1,)),
        ],
    )(
        pltpu.with_memory_space_constraint(d_nodes, pltpu.VMEM),
        pltpu.with_memory_space_constraint(gathered, pltpu.VMEM),
    )


def body(nr, nc, out_grad, node_in, weights, tile_vals, tile_rows, tile_cols, tile_count):
    relations, f = weights.shape[0], weights.shape[1]
    cap, tile = tile_vals.shape[3], tile_vals.shape[4]
    tn, width = out_grad.shape
    nd = node_in.shape[0]
    sn = nd * nc
    nz = nc // 2
    half = f // HALVES
    plane_rows = half // nr
    chunks = relations * HALVES
    assert nz % 2 == 0 and nr & (nr - 1) == 0
    places = (tn // tile) * (sn // tile)
    spread = -(-max(places, cap) // 128) * 128
    blocks = max(cap + 1, (tn // tile) * (half // tile) + (f // tile) ** 2)
    slots = relations * cap * tile // f
    assert nd == tile and slots * f == relations * cap * tile
    dma = lambda *n: pltpu.SemaphoreType.DMA(n)
    hbm = pl.BlockSpec(memory_space=pltpu.HBM)
    vmem = pl.BlockSpec(memory_space=pltpu.VMEM)
    d_nodes, gathered = pl.pallas_call(
        functools.partial(main_kernel, nr, nc, relations, sn // tile),
        out_shape=(
            pltpu.VMEM((nd, f), BF16),
            pltpu.VMEM((relations, HALVES, nr, plane_rows, f), BF16),
        ),
        in_specs=[hbm] * 7,
        out_specs=(vmem, vmem),
        scratch_shapes=[
            pltpu.VMEM(tile_rows.shape, I32),
            pltpu.VMEM(tile_cols.shape, I32),
            pltpu.VMEM((1, relations), I32),
            pltpu.VMEM((-(-2 * relations // 8) * 8, spread), I32),
            pltpu.SMEM((-(-2 * relations // 8) * 8, spread), I32),
            pltpu.VMEM((relations, blocks, tile, tile), F32),
            pltpu.VMEM((nr, tn, width), BF16),
            pltpu.VMEM((tn, f), BF16),
            pltpu.VMEM(weights.shape, BF16),
            pltpu.VMEM((relations * tn, sn), BF16),
            pltpu.VMEM((HALVES, sn, half), BF16),
            pltpu.VMEM((f, relations * tn), BF16),
            pltpu.VMEM((max(nz * 2, slots), f, nd), BF16),
            pltpu.VMEM((nz * 2, f, nd), BF16),
            pltpu.VMEM((nz + 1, 2, f, nd), BF16),
            pltpu.VMEM((nd, f), BF16),
            pltpu.VMEM((relations, HALVES, nr, plane_rows, f), BF16),
            pltpu.VMEM((relations, HALVES, nr, plane_rows, f), BF16),
            pltpu.VMEM((chunks, nr - 1, plane_rows, f), BF16),
            pltpu.VMEM((chunks, 2, plane_rows, f), BF16),
            pltpu.VMEM((chunks, 3, plane_rows, f), BF16),
            dma(4), dma(1), dma(2 + HALVES),
            dma(1), dma(1),
            dma(1), dma(HALVES, nz - 1),
            dma(1), dma(HALVES, nz),
            dma(1), dma(nz),
            dma(1), dma(nz + 1, 2),
            dma(1), dma(1),
            dma(1), dma(chunks),
            dma(1), dma(chunks),
            dma(max(nz - 1, 2)), dma(chunks, 3),
            dma(1), dma(chunks, nr - 1),
            dma(1), dma(1),
        ],
        compiler_params=pltpu.CompilerParams(
            collective_id=0, has_side_effects=True, vmem_limit_bytes=63000 * 1024
        ),
    )(
        tile_rows,
        tile_cols,
        tile_count.reshape(1, relations),
        tile_vals.reshape(slots, f, tile),
        out_grad,
        node_in,
        weights,
    )
    d_nodes, d_weights = widen(d_nodes, gathered.reshape(relations * f, f))
    return d_nodes, d_weights.reshape(relations, f, f)


def solution(mesh):
    return jax.shard_map(
        functools.partial(body, mesh.shape["row"], mesh.shape["col"]),
        mesh=mesh,
        in_specs=(
            P("col", "row"),
            P(("row", "col"), None),
            P(),
            P(None, "col", "row", None, None, None),
            P(None, "col", "row", None),
            P(None, "col", "row", None),
            P(None, "col", "row"),
        ),
        out_specs=(P(("row", "col"), None), P()),
        check_vma=False,
    )
```

```python
import functools

import jax
import jax.numpy as jnp
from jax import lax
from jax.experimental import pallas as pl
from jax.experimental.pallas import tpu as pltpu
from jax.sharding import PartitionSpec as P

MESH = pl.DeviceIdType.MESH
F32 = jnp.float32
BF16 = jnp.bfloat16
I32 = jnp.int32
HALVES = 2
WIDE = 1
scope = jax.named_scope


def reduce_order(chunks, first, half_line, wide):
    link, hop, late = 1.4, 3.6, 0.3
    events = []
    for k in range(chunks):
        t = link * k + (late if k >= first else 0.0)
        if k >= first:
            events.append((0.5 + 0.1 * k, 1, k))
        if k > 0:
            events.append((t, 2, k))
        met = t + half_line * hop + 0.4
        out = 0.3 if k < wide else (half_line - 1) * 2.8
        events += [(t + hop, 3, k), (met, 4, k), (met + out, 5, k), (met + 9.0, 6, k)]
    return [(stage, k) for _, stage, k in sorted(events)]


def main_kernel(
    nr, nc, relations, tile_cols_n,
    rows_hbm, cols_hbm, count_hbm, vals_hbm, grad_hbm, nodes_hbm, w_hbm,
    dn_ref, ag_ref,
    rows_v, cols_v, count_v, table_v, table_s, chain, gslot, g, w, a, xall, pt,
    nsend, nrecv, ndst, nfin, pbuf, crecv, precv, zbuf, zrecv,
    small_sem, val_sem, load_sem, gs, gr, xs, xr, fs, fr, ns, nrs, nzs, nzr, nfs, nfr,
    cs, cr, ps, pr, zs, zr, aps, apr, acs, acr,
):
    nz = nc // 2
    cap, tile = rows_v.shape[3], chain.shape[2]
    tn, width = gslot.shape[1], gslot.shape[2]
    nd = nodes_hbm.shape[0]
    f = w_hbm.shape[1]
    half = f // HALVES
    tile_rows_n = tn // tile
    lanes_f, lanes_h = f // tile, half // tile
    held_at = tile_rows_n * lanes_h
    plane_rows = pbuf.shape[3]
    chunks = relations * HALVES
    me_r = lax.axis_index("row")
    me_c = lax.axis_index("col")
    z = me_c // 2
    core = me_c % 2
    sibling = {"col": z * 2 + 1 - core}
    lead = core == 1
    other = core == 0

    def row_at(d):
        at, bit = me_r, 1
        while bit < nr:
            if d & bit:
                at = at + bit - 2 * bit * lax.rem(at // bit, 2)
            bit *= 2
        return at

    def row_peer(d):
        return {"row": row_at(d)}

    def z_at(k):
        return {"col": k * 2 + core}

    def z_peer(d):
        return z_at(lax.rem(z + d, nz))

    left_side = z < nz // 2
    inward = jnp.where(left_side, z + 1, z - 1)
    has_outer = (z > 0) & (z < nz - 1)
    inner = (z == nz // 2 - 1) | (z == nz // 2)
    side = jnp.where(left_side, 1, 2)
    outward = jnp.where(left_side, z - 1, z + 1)
    wide = min(WIDE, chunks)

    def remote(src, dst, send, recv, dev):
        return pltpu.make_async_remote_copy(
            src_ref=src, dst_ref=dst, send_sem=send, recv_sem=recv, device_id=dev, device_id_type=MESH
        )

    def x_slot(h, k):
        return xall.at[h, pl.ds(pl.multiple_of(k * nd, nd), nd), :]

    def x_from(d):
        return lax.rem(z + nz - d, nz) * 2 + core

    def begin(copies):
        for c in copies:
            c.start()

    with scope("entry"):
        barrier = pltpu.get_barrier_semaphore()
        for d in range(1, nr):
            pl.semaphore_signal(barrier, inc=1, device_id=row_peer(d), device_id_type=MESH)
        for d in range(1, nz):
            pl.semaphore_signal(barrier, inc=1, device_id=z_peer(d), device_id_type=MESH)
        pl.semaphore_signal(barrier, inc=1, device_id=sibling, device_id_type=MESH)

        small = [
            pltpu.make_async_copy(rows_hbm, rows_v, small_sem.at[0]),
            pltpu.make_async_copy(cols_hbm, cols_v, small_sem.at[1]),
            pltpu.make_async_copy(count_hbm, count_v, small_sem.at[2]),
        ]
        load_g = pltpu.make_async_copy(grad_hbm, gslot.at[me_r], load_sem.at[0])
        load_x = [
            pltpu.make_async_copy(nodes_hbm.at[:, h * half : (h + 1) * half], x_slot(h, me_c), load_sem.at[2 + h])
            for h in range(HALVES)
        ]
        load_w = pltpu.make_async_copy(w_hbm, w, load_sem.at[1])
        load_vals = pltpu.make_async_copy(vals_hbm, nsend.at[0 : vals_hbm.shape[0]], val_sem.at[0])
        load_g.start()
        begin(load_x)
        begin(small)
        load_vals.start()
        load_w.start()

    with scope("tables"):
        for c in small:
            c.wait()
        spread = table_v.shape[1]
        slot_lane = lax.broadcasted_iota(I32, (1, cap), 1)
        slot_row = lax.broadcasted_iota(I32, (cap, cap), 0)
        slot_col = lax.broadcasted_iota(I32, (cap, cap), 1)
        place_row = lax.broadcasted_iota(I32, (cap, spread), 0)
        place_col = lax.broadcasted_iota(I32, (cap, spread), 1)
        for r in range(relations):
            key = rows_v[r, 0] * tile_cols_n + cols_v[r, 0]
            key = jnp.where(slot_lane < count_v[0:1, r : r + 1], key, -1)
            down = jnp.max(jnp.where(slot_row == slot_col, jnp.broadcast_to(key, (cap, cap)), -1), axis=1, keepdims=True)
            same = (down == key) & (slot_row < slot_col)
            before = jnp.max(jnp.where(same, slot_row + 1, 0), axis=0, keepdims=True)
            last = jnp.max(jnp.where(down == place_col, place_row + 1, 0), axis=0, keepdims=True)
            table_v[r : r + 1, 0:cap] = before
            table_v[relations + r : relations + r + 1, :] = last
        load_table = pltpu.make_async_copy(table_v, table_s, small_sem.at[3])
        load_table.start()

    with scope("barrier"):
        pl.semaphore_wait(barrier, nr - 1 + nz - 1 + 1)
        load_g.wait()
    with scope("sends"):
        mine = gslot.at[me_r]
        begin([remote(mine, mine, gs.at[0], gr.at[0], row_peer(d)) for d in range(1, nr)])

        def send_x(h):
            load_x[h].wait()
            own = x_slot(h, me_c)

            begin([remote(own, own, xs.at[0], xr.at[h, d - 1], z_peer(d)) for d in range(1, nz)])
            remote(own, own, fs.at[0], fr.at[h, 0], sibling).start()

        send_x(0)

    with scope("chain"):
        load_table.wait()
        load_vals.wait()
        for r in range(relations):
            chain[r, 0] = jnp.zeros((tile, tile), F32)

        def link(s, carry):
            for r in range(relations):
                t = r * cap + s
                rows = pl.ds(pl.multiple_of(t % lanes_f * tile, tile), tile)
                chain[r, s + 1] = chain[r, table_s[r, s]] + nsend[t // lanes_f, rows, :].astype(F32)
            return carry

        lax.fori_loop(0, cap, link, 0)

    with scope("place"):

        def place(i, carry):
            def one(j, inner):
                for r in range(relations):
                    rows = pl.ds(pl.multiple_of(r * tn + i * tile, tile), tile)
                    cols = pl.ds(pl.multiple_of(j * tile, tile), tile)
                    a[rows, cols] = chain[r, table_s[relations + r, i * tile_cols_n + j]].astype(BF16)
                return inner

            return lax.fori_loop(0, tile_cols_n, one, carry)

        lax.fori_loop(0, tile_rows_n, place, 0)

    def forward(h, d):
        with scope(f"f{h}{d}" if isinstance(d, int) else f"f{h}"):
            slot = x_slot(h, x_from(d))
            remote(slot, slot, xs.at[0], xr.at[h, d - 1], sibling).wait_recv()
            remote(slot, slot, fs.at[0], fr.at[h, d], sibling).start()

    segments = max(tn // f, 1)
    seg = tn // segments

    def y_block(h, d):
        with scope(f"y{h}{d}"):
            slot = x_slot(h, me_c)
            remote(slot, slot, fs.at[0], fr.at[h, d], sibling).wait_recv()
            both = pl.ds(pl.multiple_of(lax.rem(z + nz - d, nz) * 2 * nd, 2 * nd), 2 * nd)
            for r in range(relations):
                part = jnp.dot(a[r * tn : (r + 1) * tn, both], xall[h, both, :], preferred_element_type=F32)
                for i in range(tile_rows_n):
                    for j in range(lanes_h):
                        b = part[i * tile : (i + 1) * tile, j * tile : (j + 1) * tile]
                        at = i * lanes_h + j
                        if d > 0:
                            b = b + chain[r, at]
                        if d < nz - 1:
                            chain[r, at] = b
                        else:
                            top = (i * tile // seg) * half + j * tile
                            side = (i * tile) % seg
                            w[r, top : top + tile, side : side + tile] = b.astype(BF16).T

    def c_copy(k):
        r, h = k % relations, k // relations
        return remote(pbuf.at[r, h], crecv.at[r, h], cs.at[0], cr.at[k], sibling)

    def held_rows(r, h, q):
        first = h * half + q * plane_rows
        block, off = first // tile, first % tile
        assert off + plane_rows <= tile
        return jnp.concatenate(
            [chain[r, held_at + block * lanes_f + j, off : off + plane_rows, :] for j in range(lanes_f)], axis=1
        )

    def terms(k):
        r, h = k % relations, k // relations
        with scope(f"terms{k}"):
            v = jnp.dot(w[r, 0:half, 0:seg], g[0:seg, :], preferred_element_type=F32)
            for s in range(1, segments):
                v = v + jnp.dot(
                    w[r, s * half : (s + 1) * half, 0:seg], g[s * seg : (s + 1) * seg, :], preferred_element_type=F32
                )
            for i in range(lanes_h):
                for j in range(lanes_f):
                    at = held_at + (h * lanes_h + i) * lanes_f + j
                    chain[r, at] = v[i * tile : (i + 1) * tile, j * tile : (j + 1) * tile]

            @pl.when(other)
            def _():
                for q in range(nr):
                    pbuf[r, h, q] = held_rows(r, h, q).astype(BF16)
                c_copy(k).start()

    def plane_scatter(r, h):
        k = h * relations + r
        with scope(f"s1_h{h}"):
            remote(pbuf.at[r, h], crecv.at[r, h], cs.at[0], cr.at[k], sibling).wait_recv()
            for q in range(nr):
                pbuf[r, h, q] = (held_rows(r, h, q) + crecv[r, h, q].astype(F32)).astype(BF16)
            begin([
                remote(pbuf.at[r, h, row_at(d)], precv.at[k, d - 1], ps.at[0], pr.at[k], row_peer(d))
                for d in range(1, nr)
            ])

    def pa_copies(k):
        part = ag_ref.at[k % relations, k // relations, me_r]
        return [remote(part, part, aps.at[0], apr.at[k, d - 1], row_peer(d)) for d in range(1, nr)]

    def ca_copy(k, d):
        part = ag_ref.at[k % relations, k // relations, row_at(d)]
        return remote(part, part, acs.at[0], acr.at[0], sibling)

    def z_hand(k, held):
        sent = zbuf.at[k, held]

        @pl.when(inner)
        def _():
            if k < wide:
                for d in range(1, nz):
                    remote(sent, zrecv.at[k, side], zs.at[d - 1], zr.at[k, side], z_peer(d)).start()
            else:
                remote(sent, zrecv.at[k, side], zs.at[0], zr.at[k, side], z_at(inward)).start()

        @pl.when(jnp.logical_not(inner))
        def _():
            remote(sent, zrecv.at[k, 0], zs.at[0], zr.at[k, 0], z_at(inward)).start()

    def z_came(k, slot):
        remote(zrecv.at[k, slot], zrecv.at[k, slot], zs.at[0], zr.at[k, slot], sibling).wait_recv()

    def plane_sum(k):
        r, h = k % relations, k // relations
        remote(precv.at[k], precv.at[k], ps.at[0], pr.at[k], sibling).wait_recv()
        part = pbuf[r, h, me_r].astype(F32)
        for d in range(1, nr):
            part = part + precv[k, d - 1].astype(F32)
        zbuf[k, 0] = part.astype(BF16)

        @pl.when(jnp.logical_not(has_outer))
        def _():
            z_hand(k, 0)

    def z_sum(k):
        @pl.when(has_outer)
        def _():
            z_came(k, 0)
            zbuf[k, 1] = (zbuf[k, 0].astype(F32) + zrecv[k, 0].astype(F32)).astype(BF16)
            z_hand(k, 1)

    def z_out(k):
        part = ag_ref.at[k % relations, k // relations, me_r]
        return remote(part, part, zs.at[1], zr.at[k, 1], z_at(outward))

    def gather_on(k):
        begin(pa_copies(k))
        ca_copy(k, 0).start()

    def inner_gather(k):
        @pl.when(inner)
        def _():
            z_came(k, 3 - side)
            own = zbuf[k, jnp.where(has_outer, 1, 0)].astype(F32)
            ag_ref[k % relations, k // relations, me_r] = (own + zrecv[k, 3 - side].astype(F32)).astype(BF16)
            if k >= wide:
                pl.when(has_outer)(lambda: z_out(k).start())
            gather_on(k)

    def outer_gather(k):
        @pl.when(jnp.logical_not(inner))
        def _():
            if k < wide:
                z_came(k, 1)
                z_came(k, 2)
                both = zrecv[k, 1].astype(F32) + zrecv[k, 2].astype(F32)
                ag_ref[k % relations, k // relations, me_r] = both.astype(BF16)
            else:
                z_out(k).wait_recv()
                pl.when(has_outer)(lambda: z_out(k).start())
            gather_on(k)

    def core_gather(k):
        copies = pa_copies(k)
        for d in range(1, nr):
            copies[d - 1].wait_recv()
            ca_copy(k, d).start()

    def mix(k, carry):
        cols = pl.ds(pl.multiple_of(k * 2 * nd, 2 * nd), 2 * nd)
        both = jnp.dot(pt[...], a[:, cols], preferred_element_type=F32)
        nsend[k * 2] = both[:, :nd].astype(BF16)
        nsend[k * 2 + 1] = both[:, nd:].astype(BF16)
        return carry

    def n_core(k):
        span = pl.ds(2 * k, 2)
        return remote(nsend.at[span], nrecv.at[span], ns.at[0], nrs.at[k], sibling)

    def dn_send(k, p, slot, to):
        remote(nsend.at[k * 2 + p], ndst.at[slot, p], nzs.at[0], nzr.at[slot, p], z_at(to)).start()

    def dn_arrived(slot, p):
        came = ndst.at[slot, p]
        remote(came, came, nzs.at[0], nzr.at[slot, p], sibling).wait_recv()

    def dn_total(k, p):
        return nsend[k * 2 + p].astype(F32) + nrecv[k * 2 + p].astype(F32)

    at_end = (z == 0) | (z == nz - 1)

    def dn_first(k):
        n_core(k).wait_recv()
        for p in range(2):
            nsend[k * 2 + p] = dn_total(k, p).astype(BF16)

            @pl.when(z == 0)
            def _():
                dn_send(k, p, k + 1, 1)

            @pl.when(z > 0)
            def _():
                dn_send(k, p, k, nz - 2)

    def dn_pass(k, p, slot, to):
        dn_arrived(slot, p)
        nsend[k * 2 + p] = (dn_total(k, p) + ndst[slot, p].astype(F32)).astype(BF16)
        dn_send(k, p, slot, to)

    def dn_up():
        def step(m, carry):
            up, p = nz - 1 - m // 2, m % 2

            @pl.when((z > 0) & (z < up))
            def _():
                dn_pass(up, p, up + 1, z + 1)

            return carry

        lax.fori_loop(0, 2 * (nz - 1), step, 0)

    def dn_down():
        def step(m, carry):
            down, p = m // 2, m % 2

            @pl.when((z > down) & (z < nz - 1))
            def _():
                dn_pass(down, p, down, z - 1)

            return carry

        lax.fori_loop(0, 2 * (nz - 1), step, 0)

    def dn_rest():
        @pl.when(left_side)
        def _():
            dn_up()
            dn_down()

        @pl.when(jnp.logical_not(left_side))
        def _():
            dn_down()
            dn_up()

    own_dn = lambda: remote(nfin, dn_ref, nfs.at[0], nfr.at[0], sibling)

    y_block(0, 0)
    if nz > 1:
        forward(0, 1)
        y_block(0, 1)
    for h in range(1, HALVES):
        with scope("sends1"):
            send_x(h)
    with scope("waitg"):
        load_w.wait()
        slots = gslot.at[0 : nr - 1]
        remote(slots, slots, gs.at[0], gr.at[0], sibling).wait_recv()
    with scope("premix"):
        for k in range(nr):
            g[:, k * width : (k + 1) * width] = gslot[k]
        for r in range(relations):
            pt[:, r * tn : (r + 1) * tn] = lax.dot_general(
                w[r], g[...], (((1,), (1,)), ((), ())), preferred_element_type=F32
            ).astype(BF16)

    def far_first(i):
        return jnp.where(left_side, nz - 1 - i, i)

    def lead_mix(i, carry):
        k = far_first(i)
        mix(k, carry)
        n_core(k).start()
        return carry

    def other_mix(i, carry):
        k = far_first(i)
        mix(k, carry)

        @pl.when(at_end & (k != z))
        def _():
            dn_first(k)

        @pl.when(i > 0)
        def _():
            forward(1, i)

        return carry

    for d in range(2, nz):
        forward(0, d)

    @pl.when(lead)
    def _():
        with scope("mix"):
            lax.fori_loop(0, nz, lead_mix, 0)

    for d in range(2, nz):
        y_block(0, d)
    for k in range(relations):
        terms(k)

        @pl.when(lead)
        def _():
            plane_scatter(k, 0)

    @pl.when(lead)
    def _():
        for d in range(1, nz):
            forward(1, d)

    @pl.when(other)
    def _():
        with scope("mix"):
            lax.fori_loop(0, nz, other_mix, 0)

    for d in range(nz):
        y_block(1, d)

    @pl.when(lead)
    def _():
        with scope("s2_0"):
            plane_sum(0)

    for k in range(relations, chunks):
        terms(k)

    stages = {
        1: lambda k: plane_scatter(k - relations, 1),
        2: plane_sum,
        3: z_sum,
        4: inner_gather,
        5: outer_gather,
        6: core_gather,
    }

    @pl.when(lead)
    def _():
        for stage, k in reduce_order(chunks, relations, nz // 2, wide):
            with scope(f"s{stage}_{k}"):
                stages[stage](k)
        with scope("end"):
            own_dn().wait_recv()
            sent = nsend.at[0 : nz * 2]
            for ref, sem in ((sent, ns), (precv, ps), (zbuf.at[:, 0], zs), (precv, aps), (ag_ref, acs)):
                remote(ref, ref, sem.at[0], sem.at[0], sibling).wait_send()

            def z_left(count, at):
                if count > 0:
                    ref = zbuf.at[0:count, 0]
                    remote(ref, ref, zs.at[at], zs.at[at], sibling).wait_send()

            @pl.when(has_outer)
            def _():
                z_left(chunks - wide, 1)

            @pl.when(inner)
            def _():
                for d in range(2, nz):
                    z_left(wide, d - 1)

    @pl.when(other)
    def _():
        def mixed(k, carry):
            @pl.when(jnp.logical_not(at_end & (k != z)))
            def _():
                n_core(k).wait_recv()

            return carry

        lax.fori_loop(0, nz, mixed, 0)
        with scope("dn_rest"):
            dn_rest()
        with scope("dn_fin"):
            for p in range(2):

                @pl.when(z > 0)
                def _():
                    dn_arrived(z + 1, p)

                @pl.when(z < nz - 1)
                def _():
                    dn_arrived(z, p)

                own = nsend[z * 2 + p].astype(F32) + nrecv[z * 2 + p].astype(F32)
                below = jnp.where(z > 0, ndst[z + 1, p].astype(F32), 0.0)
                above = jnp.where(z < nz - 1, ndst[z, p].astype(F32), 0.0)
                done = (own + below + above).T.astype(BF16)
                if p == 0:
                    dn_ref[...] = done
                else:
                    nfin[...] = done
            own_dn().start()
        with scope("oend"):
            remote(ag_ref, ag_ref, acs.at[0], acr.at[0], sibling).wait_recv()
            sent = nsend.at[0 : (nz - 1) * 2]
            for ref, sem in ((pbuf, cs), (sent, nzs), (nfin, nfs)):
                remote(ref, ref, sem.at[0], sem.at[0], sibling).wait_send()

    sent_x = xall.at[:, 0 : (nz - 1) * nd, :]
    sent_f = xall.at[:, 0 : nz * nd, :]
    for ref, sem in ((gslot.at[0 : nr - 1], gs), (sent_x, xs), (sent_f, fs)):
        remote(ref, ref, sem.at[0], sem.at[0], sibling).wait_send()


def widen_kernel(dn_ref, dw_ref, dn_out, dw_out, wide, out_sem):
    parts, rows = wide.shape[0], wide.shape[1]
    stores = [
        pltpu.make_async_copy(wide.at[k], dw_out.at[k * rows : (k + 1) * rows, :], out_sem.at[k])
        for k in range(parts)
    ]
    stores.append(pltpu.make_async_copy(dn_ref, dn_out, out_sem.at[parts]))
    stores[parts].start()
    for k in range(parts):
        wide[k] = dw_ref[k * rows : (k + 1) * rows, :].astype(F32)
        stores[k].start()
    for c in stores:
        c.wait()


def widen(d_nodes, gathered):
    total, f = gathered.shape
    parts = 6 if total % 96 == 0 else 1
    rows = total // parts
    hbm = pl.BlockSpec(memory_space=pltpu.HBM)
    vmem = pl.BlockSpec(memory_space=pltpu.VMEM)
    return pl.pallas_call(
        widen_kernel,
        in_specs=[vmem, vmem],
        out_specs=(hbm, hbm),
        out_shape=(
            jax.ShapeDtypeStruct(d_nodes.shape, BF16),
            jax.ShapeDtypeStruct(gathered.shape, F32),
        ),
        scratch_shapes=[
            pltpu.VMEM((parts, rows, f), F32),
            pltpu.SemaphoreType.DMA((parts + 1,)),
        ],
    )(
        pltpu.with_memory_space_constraint(d_nodes, pltpu.VMEM),
        pltpu.with_memory_space_constraint(gathered, pltpu.VMEM),
    )


def body(nr, nc, out_grad, node_in, weights, tile_vals, tile_rows, tile_cols, tile_count):
    relations, f = weights.shape[0], weights.shape[1]
    cap, tile = tile_vals.shape[3], tile_vals.shape[4]
    tn, width = out_grad.shape
    nd = node_in.shape[0]
    sn = nd * nc
    nz = nc // 2
    half = f // HALVES
    plane_rows = half // nr
    chunks = relations * HALVES
    assert nz % 2 == 0 and nr & (nr - 1) == 0
    places = (tn // tile) * (sn // tile)
    spread = -(-max(places, cap) // 128) * 128
    blocks = max(cap + 1, (tn // tile) * (half // tile) + (f // tile) ** 2)
    slots = relations * cap * tile // f
    assert nd == tile and slots * f == relations * cap * tile
    dma = lambda *n: pltpu.SemaphoreType.DMA(n)
    hbm = pl.BlockSpec(memory_space=pltpu.HBM)
    vmem = pl.BlockSpec(memory_space=pltpu.VMEM)
    d_nodes, gathered = pl.pallas_call(
        functools.partial(main_kernel, nr, nc, relations, sn // tile),
        out_shape=(
            pltpu.VMEM((nd, f), BF16),
            pltpu.VMEM((relations, HALVES, nr, plane_rows, f), BF16),
        ),
        in_specs=[hbm] * 7,
        out_specs=(vmem, vmem),
        scratch_shapes=[
            pltpu.VMEM(tile_rows.shape, I32),
            pltpu.VMEM(tile_cols.shape, I32),
            pltpu.VMEM((1, relations), I32),
            pltpu.VMEM((-(-2 * relations // 8) * 8, spread), I32),
            pltpu.SMEM((-(-2 * relations // 8) * 8, spread), I32),
            pltpu.VMEM((relations, blocks, tile, tile), F32),
            pltpu.VMEM((nr, tn, width), BF16),
            pltpu.VMEM((tn, f), BF16),
            pltpu.VMEM(weights.shape, BF16),
            pltpu.VMEM((relations * tn, sn), BF16),
            pltpu.VMEM((HALVES, sn, half), BF16),
            pltpu.VMEM((f, relations * tn), BF16),
            pltpu.VMEM((max(nz * 2, slots), f, nd), BF16),
            pltpu.VMEM((nz * 2, f, nd), BF16),
            pltpu.VMEM((nz + 1, 2, f, nd), BF16),
            pltpu.VMEM((nd, f), BF16),
            pltpu.VMEM((relations, HALVES, nr, plane_rows, f), BF16),
            pltpu.VMEM((relations, HALVES, nr, plane_rows, f), BF16),
            pltpu.VMEM((chunks, nr - 1, plane_rows, f), BF16),
            pltpu.VMEM((chunks, 2, plane_rows, f), BF16),
            pltpu.VMEM((chunks, 3, plane_rows, f), BF16),
            dma(4), dma(1), dma(2 + HALVES),
            dma(1), dma(1),
            dma(1), dma(HALVES, nz - 1),
            dma(1), dma(HALVES, nz),
            dma(1), dma(nz),
            dma(1), dma(nz + 1, 2),
            dma(1), dma(1),
            dma(1), dma(chunks),
            dma(1), dma(chunks),
            dma(max(nz - 1, 2)), dma(chunks, 3),
            dma(1), dma(chunks, nr - 1),
            dma(1), dma(1),
        ],
        compiler_params=pltpu.CompilerParams(
            collective_id=0, has_side_effects=True, vmem_limit_bytes=63000 * 1024
        ),
    )(
        tile_rows,
        tile_cols,
        tile_count.reshape(1, relations),
        tile_vals.reshape(slots, f, tile),
        out_grad,
        node_in,
        weights,
    )
    d_nodes, d_weights = widen(d_nodes, gathered.reshape(relations * f, f))
    return d_nodes, d_weights.reshape(relations, f, f)


def solution(mesh):
    return jax.shard_map(
        functools.partial(body, mesh.shape["row"], mesh.shape["col"]),
        mesh=mesh,
        in_specs=(
            P("col", "row"),
            P(("row", "col"), None),
            P(),
            P(None, "col", "row", None, None, None),
            P(None, "col", "row", None),
            P(None, "col", "row", None),
            P(None, "col", "row"),
        ),
        out_specs=(P(("row", "col"), None), P()),
        check_vma=False,
    )
```

```python
import functools

import jax
import jax.numpy as jnp
from jax import lax
from jax.experimental import pallas as pl
from jax.experimental.pallas import tpu as pltpu
from jax.sharding import PartitionSpec as P

MESH = pl.DeviceIdType.MESH
F32 = jnp.float32
BF16 = jnp.bfloat16
I32 = jnp.int32
HALVES = 2
WIDE = 1
scope = jax.named_scope


def reduce_order(chunks, first, half_line, wide):
    link, hop, late = 1.4, 3.6, 0.3
    events = []
    for k in range(chunks):
        t = link * k + (late if k >= first else 0.0)
        if k >= first:
            events.append((0.5 + 0.1 * k, 1, k))
        if k > 0:
            events.append((t, 2, k))
        met = t + half_line * hop + 0.4
        out = 0.3 if k < wide else (half_line - 1) * 2.8
        events += [(t + hop, 3, k), (met, 4, k), (met + out, 5, k), (met + 9.0, 6, k)]
    return [(stage, k) for _, stage, k in sorted(events)]


def main_kernel(
    nr, nc, relations, tile_cols_n,
    rows_hbm, cols_hbm, count_hbm, vals_hbm, grad_hbm, nodes_hbm, w_hbm,
    dn_ref, ag_ref,
    rows_v, cols_v, count_v, table_v, table_s, chain, gslot, g, w, a, xall, pt,
    nsend, nrecv, ndst, nfin, pbuf, crecv, precv, zbuf, zrecv,
    small_sem, val_sem, load_sem, gs, gr, xs, xr, fs, fr, ns, nrs, nzs, nzr, nfs, nfr,
    cs, cr, ps, pr, zs, zr, aps, apr, acs, acr,
):
    nz = nc // 2
    cap, tile = rows_v.shape[3], chain.shape[2]
    tn, width = gslot.shape[1], gslot.shape[2]
    nd = nodes_hbm.shape[0]
    f = w_hbm.shape[1]
    half = f // HALVES
    tile_rows_n = tn // tile
    lanes_f, lanes_h = f // tile, half // tile
    held_at = tile_rows_n * lanes_h
    plane_rows = pbuf.shape[3]
    chunks = relations * HALVES
    me_r = lax.axis_index("row")
    me_c = lax.axis_index("col")
    z = me_c // 2
    core = me_c % 2
    sibling = {"col": z * 2 + 1 - core}
    lead = core == 1
    other = core == 0

    def row_at(d):
        at, bit = me_r, 1
        while bit < nr:
            if d & bit:
                at = at + bit - 2 * bit * lax.rem(at // bit, 2)
            bit *= 2
        return at

    def row_peer(d):
        return {"row": row_at(d)}

    def z_at(k):
        return {"col": k * 2 + core}

    def z_peer(d):
        return z_at(lax.rem(z + d, nz))

    left_side = z < nz // 2
    inward = jnp.where(left_side, z + 1, z - 1)
    has_outer = (z > 0) & (z < nz - 1)
    inner = (z == nz // 2 - 1) | (z == nz // 2)
    side = jnp.where(left_side, 1, 2)
    outward = jnp.where(left_side, z - 1, z + 1)
    wide = min(WIDE, chunks)

    def remote(src, dst, send, recv, dev):
        return pltpu.make_async_remote_copy(
            src_ref=src, dst_ref=dst, send_sem=send, recv_sem=recv, device_id=dev, device_id_type=MESH
        )

    def x_slot(h, k):
        return xall.at[h, pl.ds(pl.multiple_of(k * nd, nd), nd), :]

    def x_from(d):
        return lax.rem(z + nz - d, nz) * 2 + core

    def begin(copies):
        for c in copies:
            c.start()

    with scope("entry"):
        barrier = pltpu.get_barrier_semaphore()
        for d in range(1, nr):
            pl.semaphore_signal(barrier, inc=1, device_id=row_peer(d), device_id_type=MESH)
        for d in range(1, nz):
            pl.semaphore_signal(barrier, inc=1, device_id=z_peer(d), device_id_type=MESH)
        pl.semaphore_signal(barrier, inc=1, device_id=sibling, device_id_type=MESH)

        small = [
            pltpu.make_async_copy(rows_hbm, rows_v, small_sem.at[0]),
            pltpu.make_async_copy(cols_hbm, cols_v, small_sem.at[1]),
            pltpu.make_async_copy(count_hbm, count_v, small_sem.at[2]),
        ]
        load_g = pltpu.make_async_copy(grad_hbm, gslot.at[me_r], load_sem.at[0])
        load_x = [
            pltpu.make_async_copy(nodes_hbm.at[:, h * half : (h + 1) * half], x_slot(h, me_c), load_sem.at[2 + h])
            for h in range(HALVES)
        ]
        load_w = pltpu.make_async_copy(w_hbm, w, load_sem.at[1])
        load_vals = pltpu.make_async_copy(vals_hbm, nsend.at[0 : vals_hbm.shape[0]], val_sem.at[0])
        load_g.start()
        begin(load_x)
        begin(small)
        load_vals.start()
        load_w.start()

    with scope("tables"):
        for c in small:
            c.wait()
        spread = table_v.shape[1]
        slot_lane = lax.broadcasted_iota(I32, (1, cap), 1)
        slot_row = lax.broadcasted_iota(I32, (cap, cap), 0)
        slot_col = lax.broadcasted_iota(I32, (cap, cap), 1)
        place_row = lax.broadcasted_iota(I32, (cap, spread), 0)
        place_col = lax.broadcasted_iota(I32, (cap, spread), 1)
        for r in range(relations):
            key = rows_v[r, 0] * tile_cols_n + cols_v[r, 0]
            key = jnp.where(slot_lane < count_v[0:1, r : r + 1], key, -1)
            down = jnp.max(jnp.where(slot_row == slot_col, jnp.broadcast_to(key, (cap, cap)), -1), axis=1, keepdims=True)
            same = (down == key) & (slot_row < slot_col)
            before = jnp.max(jnp.where(same, slot_row + 1, 0), axis=0, keepdims=True)
            last = jnp.max(jnp.where(down == place_col, place_row + 1, 0), axis=0, keepdims=True)
            table_v[r : r + 1, 0:cap] = before
            table_v[relations + r : relations + r + 1, :] = last
        load_table = pltpu.make_async_copy(table_v, table_s, small_sem.at[3])
        load_table.start()

    with scope("barrier"):
        pl.semaphore_wait(barrier, nr - 1 + nz - 1 + 1)
        load_g.wait()
    with scope("sends"):
        mine = gslot.at[me_r]
        begin([remote(mine, mine, gs.at[0], gr.at[0], row_peer(d)) for d in range(1, nr)])

        def send_x(h):
            load_x[h].wait()
            own = x_slot(h, me_c)

            begin([remote(own, own, xs.at[0], xr.at[h, d - 1], z_peer(d)) for d in range(1, nz)])
            remote(own, own, fs.at[0], fr.at[h, 0], sibling).start()

        send_x(0)

    with scope("chain"):
        load_table.wait()
        load_vals.wait()
        for r in range(relations):
            chain[r, 0] = jnp.zeros((tile, tile), F32)

        def link(s, carry):
            for r in range(relations):
                t = r * cap + s
                rows = pl.ds(pl.multiple_of(t % lanes_f * tile, tile), tile)
                chain[r, s + 1] = chain[r, table_s[r, s]] + nsend[t // lanes_f, rows, :].astype(F32)
            return carry

        lax.fori_loop(0, cap, link, 0)

    with scope("place"):

        def place(i, carry):
            def one(j, inner):
                for r in range(relations):
                    rows = pl.ds(pl.multiple_of(r * tn + i * tile, tile), tile)
                    cols = pl.ds(pl.multiple_of(j * tile, tile), tile)
                    a[rows, cols] = chain[r, table_s[relations + r, i * tile_cols_n + j]].astype(BF16)
                return inner

            return lax.fori_loop(0, tile_cols_n, one, carry)

        lax.fori_loop(0, tile_rows_n, place, 0)

    def forward(h, d):
        with scope(f"f{h}{d}" if isinstance(d, int) else f"f{h}"):
            slot = x_slot(h, x_from(d))
            remote(slot, slot, xs.at[0], xr.at[h, d - 1], sibling).wait_recv()
            remote(slot, slot, fs.at[0], fr.at[h, d], sibling).start()

    segments = max(tn // f, 1)
    seg = tn // segments

    def y_block(h, d):
        with scope(f"y{h}{d}"):
            slot = x_slot(h, me_c)
            remote(slot, slot, fs.at[0], fr.at[h, d], sibling).wait_recv()
            both = pl.ds(pl.multiple_of(lax.rem(z + nz - d, nz) * 2 * nd, 2 * nd), 2 * nd)
            for r in range(relations):
                part = jnp.dot(a[r * tn : (r + 1) * tn, both], xall[h, both, :], preferred_element_type=F32)
                for i in range(tile_rows_n):
                    for j in range(lanes_h):
                        b = part[i * tile : (i + 1) * tile, j * tile : (j + 1) * tile]
                        at = i * lanes_h + j
                        if d > 0:
                            b = b + chain[r, at]
                        if d < nz - 1:
                            chain[r, at] = b
                        else:
                            top = (i * tile // seg) * half + j * tile
                            side = (i * tile) % seg
                            w[r, top : top + tile, side : side + tile] = b.astype(BF16).T

    def c_copy(k):
        r, h = k % relations, k // relations
        return remote(pbuf.at[r, h], crecv.at[r, h], cs.at[0], cr.at[k], sibling)

    def held_rows(r, h, q):
        first = h * half + q * plane_rows
        block, off = first // tile, first % tile
        assert off + plane_rows <= tile
        return jnp.concatenate(
            [chain[r, held_at + block * lanes_f + j, off : off + plane_rows, :] for j in range(lanes_f)], axis=1
        )

    def terms(k):
        r, h = k % relations, k // relations
        with scope(f"terms{k}"):
            v = jnp.dot(w[r, 0:half, 0:seg], g[0:seg, :], preferred_element_type=F32)
            for s in range(1, segments):
                v = v + jnp.dot(
                    w[r, s * half : (s + 1) * half, 0:seg], g[s * seg : (s + 1) * seg, :], preferred_element_type=F32
                )
            for i in range(lanes_h):
                for j in range(lanes_f):
                    at = held_at + (h * lanes_h + i) * lanes_f + j
                    chain[r, at] = v[i * tile : (i + 1) * tile, j * tile : (j + 1) * tile]

            @pl.when(other)
            def _():
                for q in range(nr):
                    pbuf[r, h, q] = held_rows(r, h, q).astype(BF16)
                c_copy(k).start()

    def plane_scatter(r, h):
        k = h * relations + r
        with scope(f"s1_h{h}"):
            remote(pbuf.at[r, h], crecv.at[r, h], cs.at[0], cr.at[k], sibling).wait_recv()
            for q in range(nr):
                pbuf[r, h, q] = (held_rows(r, h, q) + crecv[r, h, q].astype(F32)).astype(BF16)
            begin([
                remote(pbuf.at[r, h, row_at(d)], precv.at[k, d - 1], ps.at[0], pr.at[k], row_peer(d))
                for d in range(nr - 1, 0, -1)
            ])

    def pa_copies(k):
        part = ag_ref.at[k % relations, k // relations, me_r]
        return [remote(part, part, aps.at[0], apr.at[k, d - 1], row_peer(d)) for d in range(1, nr)]

    def ca_copy(k, d):
        part = ag_ref.at[k % relations, k // relations, row_at(d)]
        return remote(part, part, acs.at[0], acr.at[0], sibling)

    def z_hand(k, held):
        sent = zbuf.at[k, held]

        @pl.when(inner)
        def _():
            if k < wide:
                for d in range(1, nz):
                    remote(sent, zrecv.at[k, side], zs.at[d - 1], zr.at[k, side], z_peer(d)).start()
            else:
                remote(sent, zrecv.at[k, side], zs.at[0], zr.at[k, side], z_at(inward)).start()

        @pl.when(jnp.logical_not(inner))
        def _():
            remote(sent, zrecv.at[k, 0], zs.at[0], zr.at[k, 0], z_at(inward)).start()

    def z_came(k, slot):
        remote(zrecv.at[k, slot], zrecv.at[k, slot], zs.at[0], zr.at[k, slot], sibling).wait_recv()

    def plane_sum(k):
        r, h = k % relations, k // relations
        remote(precv.at[k], precv.at[k], ps.at[0], pr.at[k], sibling).wait_recv()
        part = pbuf[r, h, me_r].astype(F32)
        for d in range(1, nr):
            part = part + precv[k, d - 1].astype(F32)
        zbuf[k, 0] = part.astype(BF16)

        @pl.when(jnp.logical_not(has_outer))
        def _():
            z_hand(k, 0)

    def z_sum(k):
        @pl.when(has_outer)
        def _():
            z_came(k, 0)
            zbuf[k, 1] = (zbuf[k, 0].astype(F32) + zrecv[k, 0].astype(F32)).astype(BF16)
            z_hand(k, 1)

    def z_out(k):
        part = ag_ref.at[k % relations, k // relations, me_r]
        return remote(part, part, zs.at[1], zr.at[k, 1], z_at(outward))

    def gather_on(k):
        begin(pa_copies(k)[::-1])
        ca_copy(k, 0).start()

    def inner_gather(k):
        @pl.when(inner)
        def _():
            z_came(k, 3 - side)
            own = zbuf[k, jnp.where(has_outer, 1, 0)].astype(F32)
            ag_ref[k % relations, k // relations, me_r] = (own + zrecv[k, 3 - side].astype(F32)).astype(BF16)
            if k >= wide:
                pl.when(has_outer)(lambda: z_out(k).start())
            gather_on(k)

    def outer_gather(k):
        @pl.when(jnp.logical_not(inner))
        def _():
            if k < wide:
                z_came(k, 1)
                z_came(k, 2)
                both = zrecv[k, 1].astype(F32) + zrecv[k, 2].astype(F32)
                ag_ref[k % relations, k // relations, me_r] = both.astype(BF16)
            else:
                z_out(k).wait_recv()
                pl.when(has_outer)(lambda: z_out(k).start())
            gather_on(k)

    def core_gather(k):
        copies = pa_copies(k)
        for d in range(1, nr):
            copies[d - 1].wait_recv()
            ca_copy(k, d).start()

    def mix(k, carry):
        cols = pl.ds(pl.multiple_of(k * 2 * nd, 2 * nd), 2 * nd)
        both = jnp.dot(pt[...], a[:, cols], preferred_element_type=F32)
        nsend[k * 2] = both[:, :nd].astype(BF16)
        nsend[k * 2 + 1] = both[:, nd:].astype(BF16)
        return carry

    def n_core(k):
        span = pl.ds(2 * k, 2)
        return remote(nsend.at[span], nrecv.at[span], ns.at[0], nrs.at[k], sibling)

    def dn_send(k, p, slot, to):
        remote(nsend.at[k * 2 + p], ndst.at[slot, p], nzs.at[0], nzr.at[slot, p], z_at(to)).start()

    def dn_arrived(slot, p):
        came = ndst.at[slot, p]
        remote(came, came, nzs.at[0], nzr.at[slot, p], sibling).wait_recv()

    def dn_total(k, p):
        return nsend[k * 2 + p].astype(F32) + nrecv[k * 2 + p].astype(F32)

    at_end = (z == 0) | (z == nz - 1)

    def dn_first(k):
        n_core(k).wait_recv()
        for p in range(2):
            nsend[k * 2 + p] = dn_total(k, p).astype(BF16)

            @pl.when(z == 0)
            def _():
                dn_send(k, p, k + 1, 1)

            @pl.when(z > 0)
            def _():
                dn_send(k, p, k, nz - 2)

    def dn_pass(k, p, slot, to):
        dn_arrived(slot, p)
        nsend[k * 2 + p] = (dn_total(k, p) + ndst[slot, p].astype(F32)).astype(BF16)
        dn_send(k, p, slot, to)

    def dn_up():
        def step(m, carry):
            up, p = nz - 1 - m // 2, m % 2

            @pl.when((z > 0) & (z < up))
            def _():
                dn_pass(up, p, up + 1, z + 1)

            return carry

        lax.fori_loop(0, 2 * (nz - 1), step, 0)

    def dn_down():
        def step(m, carry):
            down, p = m // 2, m % 2

            @pl.when((z > down) & (z < nz - 1))
            def _():
                dn_pass(down, p, down, z - 1)

            return carry

        lax.fori_loop(0, 2 * (nz - 1), step, 0)

    def dn_rest():
        @pl.when(left_side)
        def _():
            dn_up()
            dn_down()

        @pl.when(jnp.logical_not(left_side))
        def _():
            dn_down()
            dn_up()

    own_dn = lambda: remote(nfin, dn_ref, nfs.at[0], nfr.at[0], sibling)

    y_block(0, 0)
    if nz > 1:
        forward(0, 1)
        y_block(0, 1)
    for h in range(1, HALVES):
        with scope("sends1"):
            send_x(h)
    with scope("waitg"):
        load_w.wait()
        slots = gslot.at[0 : nr - 1]
        remote(slots, slots, gs.at[0], gr.at[0], sibling).wait_recv()
    with scope("premix"):
        for k in range(nr):
            g[:, k * width : (k + 1) * width] = gslot[k]
        for r in range(relations):
            pt[:, r * tn : (r + 1) * tn] = lax.dot_general(
                w[r], g[...], (((1,), (1,)), ((), ())), preferred_element_type=F32
            ).astype(BF16)

    def far_first(i):
        return jnp.where(left_side, nz - 1 - i, i)

    def lead_mix(i, carry):
        k = far_first(i)
        mix(k, carry)
        n_core(k).start()
        return carry

    def other_mix(i, carry):
        k = far_first(i)
        mix(k, carry)

        @pl.when(at_end & (k != z))
        def _():
            dn_first(k)

        @pl.when(i > 0)
        def _():
            forward(1, i)

        return carry

    for d in range(2, nz):
        forward(0, d)

    @pl.when(lead)
    def _():
        with scope("mix"):
            lax.fori_loop(0, nz, lead_mix, 0)

    for d in range(2, nz):
        y_block(0, d)
    for k in range(relations):
        terms(k)

        @pl.when(lead)
        def _():
            plane_scatter(k, 0)

    @pl.when(lead)
    def _():
        for d in range(1, nz):
            forward(1, d)

    @pl.when(other)
    def _():
        with scope("mix"):
            lax.fori_loop(0, nz, other_mix, 0)

    for d in range(nz):
        y_block(1, d)

    @pl.when(lead)
    def _():
        with scope("s2_0"):
            plane_sum(0)

    for k in range(relations, chunks):
        terms(k)

    stages = {
        1: lambda k: plane_scatter(k - relations, 1),
        2: plane_sum,
        3: z_sum,
        4: inner_gather,
        5: outer_gather,
        6: core_gather,
    }

    @pl.when(lead)
    def _():
        for stage, k in reduce_order(chunks, relations, nz // 2, wide):
            with scope(f"s{stage}_{k}"):
                stages[stage](k)
        with scope("end"):
            own_dn().wait_recv()
            sent = nsend.at[0 : nz * 2]
            for ref, sem in ((sent, ns), (precv, ps), (zbuf.at[:, 0], zs), (precv, aps), (ag_ref, acs)):
                remote(ref, ref, sem.at[0], sem.at[0], sibling).wait_send()

            def z_left(count, at):
                if count > 0:
                    ref = zbuf.at[0:count, 0]
                    remote(ref, ref, zs.at[at], zs.at[at], sibling).wait_send()

            @pl.when(has_outer)
            def _():
                z_left(chunks - wide, 1)

            @pl.when(inner)
            def _():
                for d in range(2, nz):
                    z_left(wide, d - 1)

    @pl.when(other)
    def _():
        def mixed(k, carry):
            @pl.when(jnp.logical_not(at_end & (k != z)))
            def _():
                n_core(k).wait_recv()

            return carry

        lax.fori_loop(0, nz, mixed, 0)
        with scope("dn_rest"):
            dn_rest()
        with scope("dn_fin"):
            for p in range(2):

                @pl.when(z > 0)
                def _():
                    dn_arrived(z + 1, p)

                @pl.when(z < nz - 1)
                def _():
                    dn_arrived(z, p)

                own = nsend[z * 2 + p].astype(F32) + nrecv[z * 2 + p].astype(F32)
                below = jnp.where(z > 0, ndst[z + 1, p].astype(F32), 0.0)
                above = jnp.where(z < nz - 1, ndst[z, p].astype(F32), 0.0)
                done = (own + below + above).T.astype(BF16)
                if p == 0:
                    dn_ref[...] = done
                else:
                    nfin[...] = done
            own_dn().start()
        with scope("oend"):
            remote(ag_ref, ag_ref, acs.at[0], acr.at[0], sibling).wait_recv()
            sent = nsend.at[0 : (nz - 1) * 2]
            for ref, sem in ((pbuf, cs), (sent, nzs), (nfin, nfs)):
                remote(ref, ref, sem.at[0], sem.at[0], sibling).wait_send()

    sent_x = xall.at[:, 0 : (nz - 1) * nd, :]
    sent_f = xall.at[:, 0 : nz * nd, :]
    for ref, sem in ((gslot.at[0 : nr - 1], gs), (sent_x, xs), (sent_f, fs)):
        remote(ref, ref, sem.at[0], sem.at[0], sibling).wait_send()


def widen_kernel(dn_ref, dw_ref, dn_out, dw_out, wide, out_sem):
    parts, rows = wide.shape[0], wide.shape[1]
    stores = [
        pltpu.make_async_copy(wide.at[k], dw_out.at[k * rows : (k + 1) * rows, :], out_sem.at[k])
        for k in range(parts)
    ]
    stores.append(pltpu.make_async_copy(dn_ref, dn_out, out_sem.at[parts]))
    stores[parts].start()
    for k in range(parts):
        wide[k] = dw_ref[k * rows : (k + 1) * rows, :].astype(F32)
        stores[k].start()
    for c in stores:
        c.wait()


def widen(d_nodes, gathered):
    total, f = gathered.shape
    parts = 6 if total % 96 == 0 else 1
    rows = total // parts
    hbm = pl.BlockSpec(memory_space=pltpu.HBM)
    vmem = pl.BlockSpec(memory_space=pltpu.VMEM)
    return pl.pallas_call(
        widen_kernel,
        in_specs=[vmem, vmem],
        out_specs=(hbm, hbm),
        out_shape=(
            jax.ShapeDtypeStruct(d_nodes.shape, BF16),
            jax.ShapeDtypeStruct(gathered.shape, F32),
        ),
        scratch_shapes=[
            pltpu.VMEM((parts, rows, f), F32),
            pltpu.SemaphoreType.DMA((parts + 1,)),
        ],
    )(
        pltpu.with_memory_space_constraint(d_nodes, pltpu.VMEM),
        pltpu.with_memory_space_constraint(gathered, pltpu.VMEM),
    )


def body(nr, nc, out_grad, node_in, weights, tile_vals, tile_rows, tile_cols, tile_count):
    relations, f = weights.shape[0], weights.shape[1]
    cap, tile = tile_vals.shape[3], tile_vals.shape[4]
    tn, width = out_grad.shape
    nd = node_in.shape[0]
    sn = nd * nc
    nz = nc // 2
    half = f // HALVES
    plane_rows = half // nr
    chunks = relations * HALVES
    assert nz % 2 == 0 and nr & (nr - 1) == 0
    places = (tn // tile) * (sn // tile)
    spread = -(-max(places, cap) // 128) * 128
    blocks = max(cap + 1, (tn // tile) * (half // tile) + (f // tile) ** 2)
    slots = relations * cap * tile // f
    assert nd == tile and slots * f == relations * cap * tile
    dma = lambda *n: pltpu.SemaphoreType.DMA(n)
    hbm = pl.BlockSpec(memory_space=pltpu.HBM)
    vmem = pl.BlockSpec(memory_space=pltpu.VMEM)
    d_nodes, gathered = pl.pallas_call(
        functools.partial(main_kernel, nr, nc, relations, sn // tile),
        out_shape=(
            pltpu.VMEM((nd, f), BF16),
            pltpu.VMEM((relations, HALVES, nr, plane_rows, f), BF16),
        ),
        in_specs=[hbm] * 7,
        out_specs=(vmem, vmem),
        scratch_shapes=[
            pltpu.VMEM(tile_rows.shape, I32),
            pltpu.VMEM(tile_cols.shape, I32),
            pltpu.VMEM((1, relations), I32),
            pltpu.VMEM((-(-2 * relations // 8) * 8, spread), I32),
            pltpu.SMEM((-(-2 * relations // 8) * 8, spread), I32),
            pltpu.VMEM((relations, blocks, tile, tile), F32),
            pltpu.VMEM((nr, tn, width), BF16),
            pltpu.VMEM((tn, f), BF16),
            pltpu.VMEM(weights.shape, BF16),
            pltpu.VMEM((relations * tn, sn), BF16),
            pltpu.VMEM((HALVES, sn, half), BF16),
            pltpu.VMEM((f, relations * tn), BF16),
            pltpu.VMEM((max(nz * 2, slots), f, nd), BF16),
            pltpu.VMEM((nz * 2, f, nd), BF16),
            pltpu.VMEM((nz + 1, 2, f, nd), BF16),
            pltpu.VMEM((nd, f), BF16),
            pltpu.VMEM((relations, HALVES, nr, plane_rows, f), BF16),
            pltpu.VMEM((relations, HALVES, nr, plane_rows, f), BF16),
            pltpu.VMEM((chunks, nr - 1, plane_rows, f), BF16),
            pltpu.VMEM((chunks, 2, plane_rows, f), BF16),
            pltpu.VMEM((chunks, 3, plane_rows, f), BF16),
            dma(4), dma(1), dma(2 + HALVES),
            dma(1), dma(1),
            dma(1), dma(HALVES, nz - 1),
            dma(1), dma(HALVES, nz),
            dma(1), dma(nz),
            dma(1), dma(nz + 1, 2),
            dma(1), dma(1),
            dma(1), dma(chunks),
            dma(1), dma(chunks),
            dma(max(nz - 1, 2)), dma(chunks, 3),
            dma(1), dma(chunks, nr - 1),
            dma(1), dma(1),
        ],
        compiler_params=pltpu.CompilerParams(
            collective_id=0, has_side_effects=True, vmem_limit_bytes=63000 * 1024
        ),
    )(
        tile_rows,
        tile_cols,
        tile_count.reshape(1, relations),
        tile_vals.reshape(slots, f, tile),
        out_grad,
        node_in,
        weights,
    )
    d_nodes, d_weights = widen(d_nodes, gathered.reshape(relations * f, f))
    return d_nodes, d_weights.reshape(relations, f, f)


def solution(mesh):
    return jax.shard_map(
        functools.partial(body, mesh.shape["row"], mesh.shape["col"]),
        mesh=mesh,
        in_specs=(
            P("col", "row"),
            P(("row", "col"), None),
            P(),
            P(None, "col", "row", None, None, None),
            P(None, "col", "row", None),
            P(None, "col", "row", None),
            P(None, "col", "row"),
        ),
        out_specs=(P(("row", "col"), None), P()),
        check_vma=False,
    )
```

```python
import functools

import jax
import jax.numpy as jnp
from jax import lax
from jax.experimental import pallas as pl
from jax.experimental.pallas import tpu as pltpu
from jax.sharding import PartitionSpec as P

MESH = pl.DeviceIdType.MESH
F32 = jnp.float32
BF16 = jnp.bfloat16
I32 = jnp.int32
HALVES = 2
WIDE = 1
scope = jax.named_scope


def reduce_order(chunks, first, half_line, wide):
    link, hop, late = 1.4, 3.6, 0.3
    events = []
    for k in range(chunks):
        t = link * k + (late if k >= first else 0.0)
        if k >= first:
            events.append((0.5 + 0.1 * k, 1, k))
        if k > 0:
            events.append((t, 2, k))
        met = t + half_line * hop + 0.4
        out = 0.3 if k < wide else (half_line - 1) * 2.8
        events += [(t + hop, 3, k), (met, 4, k), (met + out, 5, k), (met + 9.0, 6, k)]
    return [(stage, k) for _, stage, k in sorted(events)]


def main_kernel(
    nr, nc, relations, tile_cols_n,
    rows_hbm, cols_hbm, count_hbm, vals_hbm, grad_hbm, nodes_hbm, w_hbm,
    dn_ref, ag_ref,
    rows_v, cols_v, count_v, table_v, table_s, chain, gslot, g, w, a, xall, pt,
    nsend, nrecv, ndst, nfin, pbuf, crecv, precv, zbuf, zrecv,
    small_sem, val_sem, load_sem, gs, gr, xs, xr, fs, fr, ns, nrs, nzs, nzr, nfs, nfr,
    cs, cr, ps, pr, zs, zr, aps, apr, acs, acr,
):
    nz = nc // 2
    cap, tile = rows_v.shape[3], chain.shape[2]
    tn, width = gslot.shape[1], gslot.shape[2]
    nd = nodes_hbm.shape[0]
    f = w_hbm.shape[1]
    half = f // HALVES
    tile_rows_n = tn // tile
    lanes_f, lanes_h = f // tile, half // tile
    held_at = tile_rows_n * lanes_h
    plane_rows = pbuf.shape[3]
    chunks = relations * HALVES
    me_r = lax.axis_index("row")
    me_c = lax.axis_index("col")
    z = me_c // 2
    core = me_c % 2
    sibling = {"col": z * 2 + 1 - core}
    lead = core == 1
    other = core == 0

    def row_at(d):
        at, bit = me_r, 1
        while bit < nr:
            if d & bit:
                at = at + bit - 2 * bit * lax.rem(at // bit, 2)
            bit *= 2
        return at

    def row_peer(d):
        return {"row": row_at(d)}

    def z_at(k):
        return {"col": k * 2 + core}

    def z_peer(d):
        return z_at(lax.rem(z + d, nz))

    left_side = z < nz // 2
    inward = jnp.where(left_side, z + 1, z - 1)
    has_outer = (z > 0) & (z < nz - 1)
    inner = (z == nz // 2 - 1) | (z == nz // 2)
    side = jnp.where(left_side, 1, 2)
    outward = jnp.where(left_side, z - 1, z + 1)
    wide = min(WIDE, chunks)

    def remote(src, dst, send, recv, dev):
        return pltpu.make_async_remote_copy(
            src_ref=src, dst_ref=dst, send_sem=send, recv_sem=recv, device_id=dev, device_id_type=MESH
        )

    def x_slot(h, k):
        return xall.at[h, pl.ds(pl.multiple_of(k * nd, nd), nd), :]

    def x_from(d):
        return lax.rem(z + nz - d, nz) * 2 + core

    def begin(copies):
        for c in copies:
            c.start()

    with scope("entry"):
        barrier = pltpu.get_barrier_semaphore()
        for d in range(1, nr):
            pl.semaphore_signal(barrier, inc=1, device_id=row_peer(d), device_id_type=MESH)
        for d in range(1, nz):
            pl.semaphore_signal(barrier, inc=1, device_id=z_peer(d), device_id_type=MESH)
        pl.semaphore_signal(barrier, inc=1, device_id=sibling, device_id_type=MESH)

        small = [
            pltpu.make_async_copy(rows_hbm, rows_v, small_sem.at[0]),
            pltpu.make_async_copy(cols_hbm, cols_v, small_sem.at[1]),
            pltpu.make_async_copy(count_hbm, count_v, small_sem.at[2]),
        ]
        load_g = pltpu.make_async_copy(grad_hbm, gslot.at[me_r], load_sem.at[0])
        load_x = [
            pltpu.make_async_copy(nodes_hbm.at[:, h * half : (h + 1) * half], x_slot(h, me_c), load_sem.at[2 + h])
            for h in range(HALVES)
        ]
        load_w = pltpu.make_async_copy(w_hbm, w, load_sem.at[1])
        load_vals = pltpu.make_async_copy(vals_hbm, nsend.at[0 : vals_hbm.shape[0]], val_sem.at[0])
        load_g.start()
        begin(load_x)
        begin(small)
        load_vals.start()
        load_w.start()

    with scope("tables"):
        for c in small:
            c.wait()
        spread = table_v.shape[1]
        slot_lane = lax.broadcasted_iota(I32, (1, cap), 1)
        slot_row = lax.broadcasted_iota(I32, (cap, cap), 0)
        slot_col = lax.broadcasted_iota(I32, (cap, cap), 1)
        place_row = lax.broadcasted_iota(I32, (cap, spread), 0)
        place_col = lax.broadcasted_iota(I32, (cap, spread), 1)
        for r in range(relations):
            key = rows_v[r, 0] * tile_cols_n + cols_v[r, 0]
            key = jnp.where(slot_lane < count_v[0:1, r : r + 1], key, -1)
            down = jnp.max(jnp.where(slot_row == slot_col, jnp.broadcast_to(key, (cap, cap)), -1), axis=1, keepdims=True)
            same = (down == key) & (slot_row < slot_col)
            before = jnp.max(jnp.where(same, slot_row + 1, 0), axis=0, keepdims=True)
            last = jnp.max(jnp.where(down == place_col, place_row + 1, 0), axis=0, keepdims=True)
            table_v[r : r + 1, 0:cap] = before
            table_v[relations + r : relations + r + 1, :] = last
        load_table = pltpu.make_async_copy(table_v, table_s, small_sem.at[3])
        load_table.start()

    with scope("barrier"):
        pl.semaphore_wait(barrier, nr - 1 + nz - 1 + 1)
        load_g.wait()
    with scope("sends"):
        mine = gslot.at[me_r]
        begin([remote(mine, mine, gs.at[0], gr.at[0], row_peer(d)) for d in range(1, nr)])

        def send_x(h):
            load_x[h].wait()
            own = x_slot(h, me_c)

            begin([remote(own, own, xs.at[0], xr.at[h, d - 1], z_peer(d)) for d in range(1, nz)])
            remote(own, own, fs.at[0], fr.at[h, 0], sibling).start()

        send_x(0)

    with scope("chain"):
        load_table.wait()
        load_vals.wait()
        for r in range(relations):
            chain[r, 0] = jnp.zeros((tile, tile), F32)

        def link(s, carry):
            for r in range(relations):
                t = r * cap + s
                rows = pl.ds(pl.multiple_of(t % lanes_f * tile, tile), tile)
                chain[r, s + 1] = chain[r, table_s[r, s]] + nsend[t // lanes_f, rows, :].astype(F32)
            return carry

        lax.fori_loop(0, cap, link, 0)

    with scope("place"):

        def place(i, carry):
            def one(j, inner):
                for r in range(relations):
                    rows = pl.ds(pl.multiple_of(r * tn + i * tile, tile), tile)
                    cols = pl.ds(pl.multiple_of(j * tile, tile), tile)
                    a[rows, cols] = chain[r, table_s[relations + r, i * tile_cols_n + j]].astype(BF16)
                return inner

            return lax.fori_loop(0, tile_cols_n, one, carry)

        lax.fori_loop(0, tile_rows_n, place, 0)

    def forward(h, d):
        with scope(f"f{h}{d}" if isinstance(d, int) else f"f{h}"):
            slot = x_slot(h, x_from(d))
            remote(slot, slot, xs.at[0], xr.at[h, d - 1], sibling).wait_recv()
            remote(slot, slot, fs.at[0], fr.at[h, d], sibling).start()

    segments = max(tn // f, 1)
    seg = tn // segments

    def y_block(h, d):
        with scope(f"y{h}{d}"):
            slot = x_slot(h, me_c)
            remote(slot, slot, fs.at[0], fr.at[h, d], sibling).wait_recv()
            both = pl.ds(pl.multiple_of(lax.rem(z + nz - d, nz) * 2 * nd, 2 * nd), 2 * nd)
            for r in range(relations):
                part = jnp.dot(a[r * tn : (r + 1) * tn, both], xall[h, both, :], preferred_element_type=F32)
                for i in range(tile_rows_n):
                    for j in range(lanes_h):
                        b = part[i * tile : (i + 1) * tile, j * tile : (j + 1) * tile]
                        at = i * lanes_h + j
                        if d > 0:
                            b = b + chain[r, at]
                        if d < nz - 1:
                            chain[r, at] = b
                        else:
                            top = (i * tile // seg) * half + j * tile
                            side = (i * tile) % seg
                            w[r, top : top + tile, side : side + tile] = b.astype(BF16).T

    def c_copy(k):
        r, h = k % relations, k // relations
        return remote(pbuf.at[r, h], crecv.at[r, h], cs.at[0], cr.at[k], sibling)

    def held_rows(r, h, q):
        first = h * half + q * plane_rows
        block, off = first // tile, first % tile
        assert off + plane_rows <= tile
        return jnp.concatenate(
            [chain[r, held_at + block * lanes_f + j, off : off + plane_rows, :] for j in range(lanes_f)], axis=1
        )

    def terms(k):
        r, h = k % relations, k // relations
        with scope(f"terms{k}"):
            v = jnp.dot(w[r, 0:half, 0:seg], g[0:seg, :], preferred_element_type=F32)
            for s in range(1, segments):
                v = v + jnp.dot(
                    w[r, s * half : (s + 1) * half, 0:seg], g[s * seg : (s + 1) * seg, :], preferred_element_type=F32
                )
            for i in range(lanes_h):
                for j in range(lanes_f):
                    at = held_at + (h * lanes_h + i) * lanes_f + j
                    chain[r, at] = v[i * tile : (i + 1) * tile, j * tile : (j + 1) * tile]

            @pl.when(other)
            def _():
                for q in range(nr):
                    pbuf[r, h, q] = held_rows(r, h, q).astype(BF16)
                c_copy(k).start()

    def plane_scatter(r, h):
        k = h * relations + r
        with scope(f"s1_h{h}"):
            remote(pbuf.at[r, h], crecv.at[r, h], cs.at[0], cr.at[k], sibling).wait_recv()
            for q in range(nr):
                pbuf[r, h, q] = (held_rows(r, h, q) + crecv[r, h, q].astype(F32)).astype(BF16)
            begin([
                remote(pbuf.at[r, h, row_at(d)], precv.at[k, d - 1], ps.at[0], pr.at[k], row_peer(d))
                for d in range(nr - 1, 0, -1)
            ])

    def pa_copies(k):
        part = ag_ref.at[k % relations, k // relations, me_r]
        at = lambda d: k if k < chunks - 1 else k + d - 1
        return [remote(part, part, aps.at[0], apr.at[at(d)], row_peer(d)) for d in range(1, nr)]

    def ca_copy(k, d):
        part = ag_ref.at[k % relations, k // relations, row_at(d)]
        return remote(part, part, acs.at[0], acr.at[0], sibling)

    def z_hand(k, held):
        sent = zbuf.at[k, held]

        @pl.when(inner)
        def _():
            if k < wide:
                for d in range(1, nz):
                    remote(sent, zrecv.at[k, side], zs.at[d - 1], zr.at[k, side], z_peer(d)).start()
            else:
                remote(sent, zrecv.at[k, side], zs.at[0], zr.at[k, side], z_at(inward)).start()

        @pl.when(jnp.logical_not(inner))
        def _():
            remote(sent, zrecv.at[k, 0], zs.at[0], zr.at[k, 0], z_at(inward)).start()

    def z_came(k, slot):
        remote(zrecv.at[k, slot], zrecv.at[k, slot], zs.at[0], zr.at[k, slot], sibling).wait_recv()

    def plane_sum(k):
        r, h = k % relations, k // relations
        remote(precv.at[k], precv.at[k], ps.at[0], pr.at[k], sibling).wait_recv()
        part = pbuf[r, h, me_r].astype(F32)
        for d in range(1, nr):
            part = part + precv[k, d - 1].astype(F32)
        zbuf[k, 0] = part.astype(BF16)

        @pl.when(jnp.logical_not(has_outer))
        def _():
            z_hand(k, 0)

    def z_sum(k):
        @pl.when(has_outer)
        def _():
            z_came(k, 0)
            zbuf[k, 1] = (zbuf[k, 0].astype(F32) + zrecv[k, 0].astype(F32)).astype(BF16)
            z_hand(k, 1)

    def z_out(k):
        part = ag_ref.at[k % relations, k // relations, me_r]
        return remote(part, part, zs.at[1], zr.at[k, 1], z_at(outward))

    def gather_on(k):
        begin(pa_copies(k)[::-1])
        ca_copy(k, 0).start()

    def inner_gather(k):
        @pl.when(inner)
        def _():
            z_came(k, 3 - side)
            own = zbuf[k, jnp.where(has_outer, 1, 0)].astype(F32)
            ag_ref[k % relations, k // relations, me_r] = (own + zrecv[k, 3 - side].astype(F32)).astype(BF16)
            if k >= wide:
                pl.when(has_outer)(lambda: z_out(k).start())
            gather_on(k)

    def outer_gather(k):
        @pl.when(jnp.logical_not(inner))
        def _():
            if k < wide:
                z_came(k, 1)
                z_came(k, 2)
                both = zrecv[k, 1].astype(F32) + zrecv[k, 2].astype(F32)
                ag_ref[k % relations, k // relations, me_r] = both.astype(BF16)
            else:
                z_out(k).wait_recv()
                pl.when(has_outer)(lambda: z_out(k).start())
            gather_on(k)

    def core_gather(k):
        if k < chunks - 1:
            remote(precv.at[k], precv.at[k], aps.at[0], apr.at[k], sibling).wait_recv()
            begin([ca_copy(k, d) for d in range(1, nr)])
            return
        copies = pa_copies(k)
        for d in range(1, nr):
            copies[d - 1].wait_recv()
            ca_copy(k, d).start()

    def mix(k, carry):
        cols = pl.ds(pl.multiple_of(k * 2 * nd, 2 * nd), 2 * nd)
        both = jnp.dot(pt[...], a[:, cols], preferred_element_type=F32)
        nsend[k * 2] = both[:, :nd].astype(BF16)
        nsend[k * 2 + 1] = both[:, nd:].astype(BF16)
        return carry

    def n_core(k):
        span = pl.ds(2 * k, 2)
        return remote(nsend.at[span], nrecv.at[span], ns.at[0], nrs.at[k], sibling)

    def dn_send(k, p, slot, to):
        remote(nsend.at[k * 2 + p], ndst.at[slot, p], nzs.at[0], nzr.at[slot, p], z_at(to)).start()

    def dn_arrived(slot, p):
        came = ndst.at[slot, p]
        remote(came, came, nzs.at[0], nzr.at[slot, p], sibling).wait_recv()

    def dn_total(k, p):
        return nsend[k * 2 + p].astype(F32) + nrecv[k * 2 + p].astype(F32)

    at_end = (z == 0) | (z == nz - 1)

    def dn_first(k):
        n_core(k).wait_recv()
        for p in range(2):
            nsend[k * 2 + p] = dn_total(k, p).astype(BF16)

            @pl.when(z == 0)
            def _():
                dn_send(k, p, k + 1, 1)

            @pl.when(z > 0)
            def _():
                dn_send(k, p, k, nz - 2)

    def dn_pass(k, p, slot, to):
        dn_arrived(slot, p)
        nsend[k * 2 + p] = (dn_total(k, p) + ndst[slot, p].astype(F32)).astype(BF16)
        dn_send(k, p, slot, to)

    def dn_up():
        def step(m, carry):
            up, p = nz - 1 - m // 2, m % 2

            @pl.when((z > 0) & (z < up))
            def _():
                dn_pass(up, p, up + 1, z + 1)

            return carry

        lax.fori_loop(0, 2 * (nz - 1), step, 0)

    def dn_down():
        def step(m, carry):
            down, p = m // 2, m % 2

            @pl.when((z > down) & (z < nz - 1))
            def _():
                dn_pass(down, p, down, z - 1)

            return carry

        lax.fori_loop(0, 2 * (nz - 1), step, 0)

    def dn_rest():
        @pl.when(left_side)
        def _():
            dn_up()
            dn_down()

        @pl.when(jnp.logical_not(left_side))
        def _():
            dn_down()
            dn_up()

    own_dn = lambda: remote(nfin, dn_ref, nfs.at[0], nfr.at[0], sibling)

    y_block(0, 0)
    if nz > 1:
        forward(0, 1)
        y_block(0, 1)
    for h in range(1, HALVES):
        with scope("sends1"):
            send_x(h)
    with scope("waitg"):
        load_w.wait()
        slots = gslot.at[0 : nr - 1]
        remote(slots, slots, gs.at[0], gr.at[0], sibling).wait_recv()
    with scope("premix"):
        for k in range(nr):
            g[:, k * width : (k + 1) * width] = gslot[k]
        for r in range(relations):
            pt[:, r * tn : (r + 1) * tn] = lax.dot_general(
                w[r], g[...], (((1,), (1,)), ((), ())), preferred_element_type=F32
            ).astype(BF16)

    def far_first(i):
        return jnp.where(left_side, nz - 1 - i, i)

    def lead_mix(i, carry):
        k = far_first(i)
        mix(k, carry)
        n_core(k).start()
        return carry

    def other_mix(i, carry):
        k = far_first(i)
        mix(k, carry)

        @pl.when(at_end & (k != z))
        def _():
            dn_first(k)

        @pl.when(i > 0)
        def _():
            forward(1, i)

        return carry

    for d in range(2, nz):
        forward(0, d)

    @pl.when(lead)
    def _():
        with scope("mix"):
            lax.fori_loop(0, nz, lead_mix, 0)

    for d in range(2, nz):
        y_block(0, d)
    for k in range(relations):
        terms(k)

        @pl.when(lead)
        def _():
            plane_scatter(k, 0)

    @pl.when(lead)
    def _():
        for d in range(1, nz):
            forward(1, d)

    @pl.when(other)
    def _():
        with scope("mix"):
            lax.fori_loop(0, nz, other_mix, 0)

    for d in range(nz):
        y_block(1, d)

    @pl.when(lead)
    def _():
        with scope("s2_0"):
            plane_sum(0)

    for k in range(relations, chunks):
        terms(k)

    stages = {
        1: lambda k: plane_scatter(k - relations, 1),
        2: plane_sum,
        3: z_sum,
        4: inner_gather,
        5: outer_gather,
        6: core_gather,
    }

    @pl.when(lead)
    def _():
        for stage, k in reduce_order(chunks, relations, nz // 2, wide):
            with scope(f"s{stage}_{k}"):
                stages[stage](k)
        with scope("end"):
            own_dn().wait_recv()
            sent = nsend.at[0 : nz * 2]
            for ref, sem in ((sent, ns), (precv, ps), (zbuf.at[:, 0], zs), (precv, aps), (ag_ref, acs)):
                remote(ref, ref, sem.at[0], sem.at[0], sibling).wait_send()

            def z_left(count, at):
                if count > 0:
                    ref = zbuf.at[0:count, 0]
                    remote(ref, ref, zs.at[at], zs.at[at], sibling).wait_send()

            @pl.when(has_outer)
            def _():
                z_left(chunks - wide, 1)

            @pl.when(inner)
            def _():
                for d in range(2, nz):
                    z_left(wide, d - 1)

    @pl.when(other)
    def _():
        def mixed(k, carry):
            @pl.when(jnp.logical_not(at_end & (k != z)))
            def _():
                n_core(k).wait_recv()

            return carry

        lax.fori_loop(0, nz, mixed, 0)
        with scope("dn_rest"):
            dn_rest()
        with scope("dn_fin"):
            for p in range(2):

                @pl.when(z > 0)
                def _():
                    dn_arrived(z + 1, p)

                @pl.when(z < nz - 1)
                def _():
                    dn_arrived(z, p)

                own = nsend[z * 2 + p].astype(F32) + nrecv[z * 2 + p].astype(F32)
                below = jnp.where(z > 0, ndst[z + 1, p].astype(F32), 0.0)
                above = jnp.where(z < nz - 1, ndst[z, p].astype(F32), 0.0)
                done = (own + below + above).T.astype(BF16)
                if p == 0:
                    dn_ref[...] = done
                else:
                    nfin[...] = done
            own_dn().start()
        with scope("oend"):
            remote(ag_ref, ag_ref, acs.at[0], acr.at[0], sibling).wait_recv()
            sent = nsend.at[0 : (nz - 1) * 2]
            for ref, sem in ((pbuf, cs), (sent, nzs), (nfin, nfs)):
                remote(ref, ref, sem.at[0], sem.at[0], sibling).wait_send()

    sent_x = xall.at[:, 0 : (nz - 1) * nd, :]
    sent_f = xall.at[:, 0 : nz * nd, :]
    for ref, sem in ((gslot.at[0 : nr - 1], gs), (sent_x, xs), (sent_f, fs)):
        remote(ref, ref, sem.at[0], sem.at[0], sibling).wait_send()


def widen_kernel(dn_ref, dw_ref, dn_out, dw_out, wide, out_sem):
    parts, rows = wide.shape[0], wide.shape[1]
    stores = [
        pltpu.make_async_copy(wide.at[k], dw_out.at[k * rows : (k + 1) * rows, :], out_sem.at[k])
        for k in range(parts)
    ]
    stores.append(pltpu.make_async_copy(dn_ref, dn_out, out_sem.at[parts]))
    stores[parts].start()
    for k in range(parts):
        wide[k] = dw_ref[k * rows : (k + 1) * rows, :].astype(F32)
        stores[k].start()
    for c in stores:
        c.wait()


def widen(d_nodes, gathered):
    total, f = gathered.shape
    parts = 12 if total % 192 == 0 else 1
    rows = total // parts
    hbm = pl.BlockSpec(memory_space=pltpu.HBM)
    vmem = pl.BlockSpec(memory_space=pltpu.VMEM)
    return pl.pallas_call(
        widen_kernel,
        in_specs=[vmem, vmem],
        out_specs=(hbm, hbm),
        out_shape=(
            jax.ShapeDtypeStruct(d_nodes.shape, BF16),
            jax.ShapeDtypeStruct(gathered.shape, F32),
        ),
        scratch_shapes=[
            pltpu.VMEM((parts, rows, f), F32),
            pltpu.SemaphoreType.DMA((parts + 1,)),
        ],
    )(
        pltpu.with_memory_space_constraint(d_nodes, pltpu.VMEM),
        pltpu.with_memory_space_constraint(gathered, pltpu.VMEM),
    )


def body(nr, nc, out_grad, node_in, weights, tile_vals, tile_rows, tile_cols, tile_count):
    relations, f = weights.shape[0], weights.shape[1]
    cap, tile = tile_vals.shape[3], tile_vals.shape[4]
    tn, width = out_grad.shape
    nd = node_in.shape[0]
    sn = nd * nc
    nz = nc // 2
    half = f // HALVES
    plane_rows = half // nr
    chunks = relations * HALVES
    assert nz % 2 == 0 and nr & (nr - 1) == 0
    places = (tn // tile) * (sn // tile)
    spread = -(-max(places, cap) // 128) * 128
    blocks = max(cap + 1, (tn // tile) * (half // tile) + (f // tile) ** 2)
    slots = relations * cap * tile // f
    assert nd == tile and slots * f == relations * cap * tile
    dma = lambda *n: pltpu.SemaphoreType.DMA(n)
    hbm = pl.BlockSpec(memory_space=pltpu.HBM)
    vmem = pl.BlockSpec(memory_space=pltpu.VMEM)
    d_nodes, gathered = pl.pallas_call(
        functools.partial(main_kernel, nr, nc, relations, sn // tile),
        out_shape=(
            pltpu.VMEM((nd, f), BF16),
            pltpu.VMEM((relations, HALVES, nr, plane_rows, f), BF16),
        ),
        in_specs=[hbm] * 7,
        out_specs=(vmem, vmem),
        scratch_shapes=[
            pltpu.VMEM(tile_rows.shape, I32),
            pltpu.VMEM(tile_cols.shape, I32),
            pltpu.VMEM((1, relations), I32),
            pltpu.VMEM((-(-2 * relations // 8) * 8, spread), I32),
            pltpu.SMEM((-(-2 * relations // 8) * 8, spread), I32),
            pltpu.VMEM((relations, blocks, tile, tile), F32),
            pltpu.VMEM((nr, tn, width), BF16),
            pltpu.VMEM((tn, f), BF16),
            pltpu.VMEM(weights.shape, BF16),
            pltpu.VMEM((relations * tn, sn), BF16),
            pltpu.VMEM((HALVES, sn, half), BF16),
            pltpu.VMEM((f, relations * tn), BF16),
            pltpu.VMEM((max(nz * 2, slots), f, nd), BF16),
            pltpu.VMEM((nz * 2, f, nd), BF16),
            pltpu.VMEM((nz + 1, 2, f, nd), BF16),
            pltpu.VMEM((nd, f), BF16),
            pltpu.VMEM((relations, HALVES, nr, plane_rows, f), BF16),
            pltpu.VMEM((relations, HALVES, nr, plane_rows, f), BF16),
            pltpu.VMEM((chunks, nr - 1, plane_rows, f), BF16),
            pltpu.VMEM((chunks, 2, plane_rows, f), BF16),
            pltpu.VMEM((chunks, 3, plane_rows, f), BF16),
            dma(4), dma(1), dma(2 + HALVES),
            dma(1), dma(1),
            dma(1), dma(HALVES, nz - 1),
            dma(1), dma(HALVES, nz),
            dma(1), dma(nz),
            dma(1), dma(nz + 1, 2),
            dma(1), dma(1),
            dma(1), dma(chunks),
            dma(1), dma(chunks),
            dma(max(nz - 1, 2)), dma(chunks, 3),
            dma(1), dma(chunks - 1 + nr - 1),
            dma(1), dma(1),
        ],
        compiler_params=pltpu.CompilerParams(
            collective_id=0, has_side_effects=True, vmem_limit_bytes=63000 * 1024
        ),
    )(
        tile_rows,
        tile_cols,
        tile_count.reshape(1, relations),
        tile_vals.reshape(slots, f, tile),
        out_grad,
        node_in,
        weights,
    )
    d_nodes, d_weights = widen(d_nodes, gathered.reshape(relations * f, f))
    return d_nodes, d_weights.reshape(relations, f, f)


def solution(mesh):
    return jax.shard_map(
        functools.partial(body, mesh.shape["row"], mesh.shape["col"]),
        mesh=mesh,
        in_specs=(
            P("col", "row"),
            P(("row", "col"), None),
            P(),
            P(None, "col", "row", None, None, None),
            P(None, "col", "row", None),
            P(None, "col", "row", None),
            P(None, "col", "row"),
        ),
        out_specs=(P(("row", "col"), None), P()),
        check_vma=False,
    )
```
